32 devices in a mesh: row: 8 (over z, core), col: 4 (over y, x).
Axes of the slice: x: 2, y: 2, z: 4, core: 2. Of those that a mesh axis runs over, the one named last changes fastest.
Arguments:
- schur_blocks: bfloat16 [4, 8, 8, 4, 256, 256], P(None, 'row', None, 'col'), may hold values from -0.1875 to 0.1875
- known_blocks: float32 [4, 8, 8, 4, 256, 256], P(None, 'row', None, 'col'), may hold values from -6 to 6
- eigen_pairs: float32 [4, 8, 2, 256, 256], P(None, 'row'), as said below
- eigenvalues: float32 [32, 256], replicated, may hold values from 1 to 8.95, as said below
Outputs:
- updated: float32 [4, 8, 8, 4, 256, 256], P(None, 'row', None, 'col')
The draws below stay inside these ranges and needn't reach their ends.
Inputs may be any that keep to these rules, and one draw needn't show every extreme that they name: For each block, eigen_pairs[a, r, 0] is unit upper triangular and eigen_pairs[a, r, 1] is its inverse. `eigenvalues`: row i lies within 1 + i / 4 and 1.2 + i / 4.
All inputs are finite; a program needn't handle non-finite values.
Results may differ from the reference program's by a relative error of at most 0.0017.
Values may be sent and summed in bfloat16 or wider, within the bound.
No kernel may reach another device: no remote copies, remote signals or barrier semaphores. Data moves between devices by JAX's collectives and lax.ppermute only.
A program may use at most 192 MiB of HBM per device.

```python
import math
import jax
import jax.numpy as jnp
from jax import lax

BS = 256
FIRST = 8
DIAGS = 4
BPR = 4
BPC = 8
N_ROW = 8
N_COL = 4


def draw_eigen_pairs(key, part):
    count = BPR * N_ROW
    spread = 0.32 / math.sqrt(BS)
    upper = jax.random.normal(key, (count, BS, BS), jnp.float32) * spread
    identity = jnp.eye(BS, dtype=jnp.float32)
    vectors = jnp.triu(upper, 1) + identity
    inverses = lax.linalg.triangular_solve(vectors, jnp.broadcast_to(identity, vectors.shape), left_side=True, lower=False)
    return jnp.stack([vectors, inverses], axis=1).reshape(BPR, N_ROW, 2, BS, BS)


def draw_eigenvalues(key, part):
    count = BPR * N_ROW
    base = 1.0 + 0.25 * jnp.arange(count, dtype=jnp.float32)[:, None]
    fraction = jax.random.uniform(key, (count, BS), jnp.float32)
    return base + 0.2 * fraction


def level_of(own_key, extent, shards, low, high):
    level = 1.0
    for axis_at, blocks in shards:
        draws = jax.random.uniform(jax.random.fold_in(jax.random.fold_in(own_key, 6), axis_at), (blocks,), jnp.float32, low / len(shards), high / len(shards))
        level = level * jnp.repeat(jnp.exp(draws), extent[axis_at] // blocks).reshape((-1,) + (1,) * (len(extent) - 1 - axis_at))
    return level


def noise(key, extent, scale, bound, pieces=(), held_as=jnp.bfloat16):
    entries = jax.random.normal(key, extent, jnp.float32) * scale
    if len(pieces) > 0:
        entries = level_of(key, extent, pieces, -0.22, 0.18) * entries
    return jnp.clip(entries, min=-bound, max=bound).astype(held_as)


def setup_inputs(seed: int = 0) -> dict:
    key_of = jax.random.split(jax.random.key(seed), 5)
    schur_blocks = noise(key_of[0], (BPR, N_ROW, BPC, N_COL, BS, BS), (4 * BS) ** -0.5, 0.1875, ((1, 8), (3, 4)))
    known_blocks = noise(key_of[1], (BPR, N_ROW, BPC, N_COL, BS, BS), 1.0, 6.0, ((1, 8), (3, 4)), jnp.float32)
    eigen_pairs = draw_eigen_pairs(jax.random.fold_in(key_of[4], 71), 0)
    eigenvalues = draw_eigenvalues(jax.random.fold_in(key_of[4], 71), 0)
    return dict(schur_blocks=schur_blocks, known_blocks=known_blocks, eigen_pairs=eigen_pairs, eigenvalues=eigenvalues)


def full_dot(left_side, right_side):
    return jnp.dot(left_side.astype(jnp.float32), right_side.astype(jnp.float32), precision=lax.Precision.HIGHEST, preferred_element_type=jnp.float32)

def reference(schur_blocks, known_blocks, eigen_pairs, eigenvalues):
    blocks_total = BPR * N_ROW

    def schur_at(row_block, col_block):
        return schur_blocks[row_block // N_ROW, row_block % N_ROW, col_block // N_COL, col_block % N_COL]
    rounded = {}

    def factor_at(row_block, col_block):
        if (row_block, col_block) in rounded:
            return rounded[row_block, col_block]
        return known_blocks[row_block // N_ROW, row_block % N_ROW, col_block // N_COL, col_block % N_COL].astype(jnp.bfloat16)
    placed_blocks = []
    first_major = []
    first_minor = []
    second_major = []
    second_minor = []
    for distance in range(FIRST, FIRST + DIAGS):
        for row_block in range(blocks_total - distance):
            col_block = row_block + distance
            running = jnp.zeros((BS, BS), jnp.float32)
            for middle in range(row_block, col_block):
                running = running + jnp.dot(factor_at(row_block, middle).astype(jnp.float32), schur_at(middle, col_block).astype(jnp.float32), preferred_element_type=jnp.float32)
            for middle in range(row_block + 1, col_block + 1):
                running = running - jnp.dot(schur_at(row_block, middle).astype(jnp.float32), factor_at(middle, col_block).astype(jnp.float32), preferred_element_type=jnp.float32)
            pair_left = eigen_pairs[row_block // N_ROW, row_block % N_ROW]
            pair_right = eigen_pairs[col_block // N_ROW, col_block % N_ROW]
            spacing = eigenvalues[row_block][:, None] - eigenvalues[col_block][None, :]
            mixed_block = full_dot(full_dot(pair_left[1], running), pair_right[0]) / spacing
            solved = full_dot(full_dot(pair_left[0], mixed_block), pair_right[1])
            rounded[row_block, col_block] = solved.astype(jnp.bfloat16)
            placed_blocks.append(solved)
            first_major.append(row_block // N_ROW)
            first_minor.append(row_block % N_ROW)
            second_major.append(col_block // N_COL)
            second_minor.append(col_block % N_COL)
    index_one = jnp.array(first_major).astype(jnp.int32)
    index_two = jnp.array(first_minor).astype(jnp.int32)
    index_three = jnp.array(second_major).astype(jnp.int32)
    index_four = jnp.array(second_minor).astype(jnp.int32)
    return known_blocks.at[index_one, index_two, index_three, index_four].set(jnp.stack(placed_blocks))
```

```python
import functools

import jax
import jax.numpy as jnp
from jax import lax
from jax.experimental import pallas as pl
from jax.experimental.pallas import tpu as pltpu
from jax.sharding import PartitionSpec as P

FIRST = 8
DIAGS = 4


def shifted(block, axis, distance):
    devices = range(lax.axis_size(axis))
    route = [((i - distance) % len(devices), i) for i in devices]
    return lax.ppermute(block, axis, route)


def pick_rows(stacked, indices):
    return jax.vmap(lambda source, chosen: source[chosen])(stacked, indices)


def full_dot(left_side, right_side):
    return jnp.einsum(
        "apq,aqr->apr",
        left_side,
        right_side,
        precision=lax.Precision.HIGHEST,
        preferred_element_type=jnp.float32,
    )


def right_terms(known_rows, schur_rows, known_cols, schur_cols, offsets, usable, distance):
    band_width = known_rows.shape[1]
    reach_back = distance[:, :, None] - offsets
    first_mask = usable & (offsets >= 1) & (reach_back >= 0) & (reach_back <= FIRST - 1)
    second_mask = usable & (offsets <= FIRST - 1) & (reach_back >= 1)
    clipped = jnp.clip(reach_back, 0, band_width - 1)
    known_pick = jnp.where(first_mask[..., None, None], pick_rows(known_rows, clipped), 0)
    schur_pick = jnp.where(second_mask[..., None, None], -pick_rows(schur_rows, clipped), 0)
    left_side = jnp.concatenate([known_pick, schur_pick], axis=2)
    right_side = jnp.concatenate([schur_cols, known_cols], axis=2)
    return jnp.einsum(
        "atepq,ateqr->atpr", left_side, right_side, preferred_element_type=jnp.float32
    )


def body(schur_blocks, known_blocks, eigen_pairs, eigenvalues):
    row_count = lax.axis_size("row")
    col_count = lax.axis_size("col")
    row_index = lax.axis_index("row")
    col_index = lax.axis_index("col")
    schur_local = schur_blocks[:, 0, :, 0]
    known_local = known_blocks[:, 0, :, 0]
    pairs_local = eigen_pairs[:, 0]
    block_rows = schur_local.shape[0]
    block_cols = schur_local.shape[1]
    blocks_total = block_rows * row_count
    band_width = FIRST + DIAGS
    row_slots = -(-band_width // col_count)
    col_slots = -(-band_width // row_count)
    per_row = -(-DIAGS // col_count)
    row_ids = jnp.arange(block_rows, dtype=jnp.int32) * row_count + row_index
    col_ids = jnp.arange(block_cols, dtype=jnp.int32) * col_count + col_index
    band_range = jnp.arange(band_width, dtype=jnp.int32)
    row_range = jnp.arange(block_rows, dtype=jnp.int32)
    row_offsets = (
        jnp.mod(col_index - row_ids, col_count)[:, None]
        + jnp.arange(row_slots, dtype=jnp.int32)[None, :] * col_count
    )
    row_reach = row_ids[:, None] + row_offsets
    row_valid = (row_offsets < band_width) & (row_reach < blocks_total)
    row_pick = jnp.clip(row_reach // col_count, 0, block_cols - 1)
    known_send = jnp.where(
        row_valid[..., None, None], pick_rows(known_local, row_pick), 0.0
    ).astype(jnp.bfloat16)
    schur_send = jnp.where(row_valid[..., None, None], pick_rows(schur_local, row_pick), 0)
    known_recv, schur_recv = (
        lax.all_gather(known_send[None], "col", axis=0, tiled=True),
        lax.all_gather(schur_send[None], "col", axis=0, tiled=True),
    )
    row_source = jnp.mod(row_ids[:, None] + band_range[None, :], col_count)
    row_slot = (band_range // col_count)[None, :]
    known_rows = known_recv[row_source, row_range[:, None], row_slot]
    schur_rows = schur_recv[row_source, row_range[:, None], row_slot]
    col_offsets = (
        jnp.mod(col_ids - row_index, row_count)[:, None]
        + jnp.arange(col_slots, dtype=jnp.int32)[None, :] * row_count
    )
    col_reach = col_ids[:, None] - col_offsets
    col_valid = (col_offsets < band_width) & (col_reach >= 0)
    col_pick = jnp.clip(col_reach // row_count, 0, block_rows - 1)
    known_down = jnp.where(
        col_valid[..., None, None], pick_rows(jnp.swapaxes(known_local, 0, 1), col_pick), 0.0
    ).astype(jnp.bfloat16)
    schur_down = jnp.where(
        col_valid[..., None, None], pick_rows(jnp.swapaxes(schur_local, 0, 1), col_pick), 0
    )
    target_first = -((col_index - row_ids - FIRST) // col_count)
    target_block = target_first[:, None] + jnp.arange(per_row, dtype=jnp.int32)[None, :]
    target_cols = target_block * col_count + col_index
    distance = target_cols - row_ids[:, None]
    active = (target_block < block_cols) & (distance <= FIRST + DIAGS - 1)
    target_clip = jnp.clip(target_block, 0, block_cols - 1)
    own_strip = jnp.stack([known_down, schur_down])
    collected = jnp.zeros((row_count,) + own_strip.shape, jnp.bfloat16)
    collected = collected.at[row_index].set(own_strip)
    reach_rows = min(row_count, band_width)
    carried = own_strip
    for step in range(1, reach_rows):
        carried = shifted(carried, "row", row_count - 1)
        collected = collected.at[jnp.mod(row_index + step, row_count)].set(carried)
    known_all = collected[:, 0]
    schur_all = collected[:, 1]
    col_source = jnp.mod(target_cols[:, :, None] - band_range[None, None, :], row_count)
    col_slot = (band_range // row_count)[None, None, :]
    known_cols = known_all[col_source, target_clip[:, :, None], col_slot]
    schur_cols = schur_all[col_source, target_clip[:, :, None], col_slot]
    offsets = jnp.broadcast_to(band_range[None, None, :], col_source.shape)
    totals = right_terms(
        known_rows,
        schur_rows,
        known_cols,
        schur_cols,
        offsets,
        jnp.ones(offsets.shape, jnp.bool_),
        distance,
    )
    kept_cols = schur_cols[:, :, :DIAGS]
    pair_list = []
    for distance_now in range(FIRST, FIRST + DIAGS):
        lag = distance_now % row_count
        receiver = jnp.mod(row_index - lag, row_count)
        wanted = jnp.clip(
            (row_range * row_count + receiver + distance_now) // row_count, 0, block_rows - 1
        )
        sending = pairs_local[wanted]
        if lag == 0:
            pair_list.append(sending)
        else:
            pair_list.append(
                shifted(sending.astype(jnp.bfloat16), "row", row_count - lag).astype(sending.dtype)
            )
    vec_left = pairs_local[:, 0]
    inv_left = pairs_local[:, 1]
    lam_left = eigenvalues[row_ids]
    output = known_local
    for distance_now in range(FIRST, FIRST + DIAGS):
        hitting = active & (distance == distance_now)
        solving = jnp.any(hitting, axis=1)
        chosen = jnp.sum(jnp.where(hitting[..., None, None], totals, 0.0), axis=1)
        block_col = jnp.sum(jnp.where(hitting, target_clip, 0), axis=1)
        block_ids = jnp.clip(block_col * col_count + col_index, 0, blocks_total - 1)
        vec_right = pair_list[distance_now - FIRST][:, 0]
        inv_right = pair_list[distance_now - FIRST][:, 1]
        lam_right = eigenvalues[block_ids]
        spacing = lam_left[:, :, None] - lam_right[:, None, :]
        spacing = jnp.where(solving[:, None, None], spacing, 1.0)
        mixed_block = full_dot(full_dot(inv_left, chosen), vec_right) / spacing
        solved = full_dot(full_dot(vec_left, mixed_block), inv_right)
        solved = jnp.where(solving[:, None, None], solved, 0.0)
        placing = solving[:, None] & (
            jnp.arange(block_cols, dtype=jnp.int32)[None, :] == block_col[:, None]
        )
        output = jnp.where(placing[:, :, None, None], solved[:, None], output)
        if distance_now < FIRST + DIAGS - 1:
            rounded = solved.astype(jnp.bfloat16)
            for gap in range(1, FIRST + DIAGS - distance_now):
                row_new = shifted(rounded, "col", gap)
                receiver = jnp.mod(row_index - gap, row_count)
                wanted = jnp.clip(
                    (row_range * row_count + receiver + gap) // row_count, 0, block_rows - 1
                )
                col_new = shifted(rounded[wanted], "row", row_count - gap)
                growing = active & (distance - distance_now == gap)
                known_from_row = row_new[:, None]
                known_from_col = col_new[:, None]
                schur_from_row = schur_rows[:, gap][:, None]
                schur_from_col = kept_cols[:, :, gap]
                left_side = jnp.stack(
                    [
                        jnp.where(growing[..., None, None], known_from_row, 0),
                        jnp.where(growing[..., None, None], -schur_from_row, 0),
                    ],
                    axis=2,
                )
                right_side = jnp.stack([schur_from_col, known_from_col], axis=2)
                totals = totals + jnp.einsum(
                    "atepq,ateqr->atpr", left_side, right_side, preferred_element_type=jnp.float32
                )
    return output[:, None, :, None]


def lag_of(r, c, cols):
    return lax.rem(c - r + 2 * cols * FIRST, cols)


def lead_of(r, c, cols):
    return lax.div(r - c + lag_of(r, c, cols), cols)


def any_spec():
    return pl.BlockSpec(memory_space=pl.ANY)


def place_spec():
    return pl.BlockSpec(memory_space=pltpu.SMEM)


def mod_add(value, shift, size):
    return lax.rem(value + shift + 4 * size, size)


def column_picks(place, step, chips, aim_core, rows, cols, a):
    r, c = place[0], place[1]
    chip = mod_add(lax.div(r, 2), -step, chips)
    lead = lead_of(2 * chip + aim_core, c, cols)
    j = rows * a + FIRST + cols * lead + c
    off_f = lax.rem(j - r + rows, rows)
    off_s = 1 + lax.rem(j - r - 1 + rows, rows)
    return lax.div(j - off_f - r, rows), lax.div(j - off_s - r, rows), (j - c) // cols


def pack(known, schur, place, aim_core, rows, cols, with_rows):
    block_rows, block_cols, bs = known.shape[0], known.shape[1], known.shape[2]
    count = block_rows - 1
    chips = rows // 2
    slots = FIRST // cols
    lead_steps = count * slots if with_rows else 0

    def source(n, place):
        r, c = place[0], place[1]
        m = jnp.maximum(n - lead_steps, 0)
        f_row, s_row, b = column_picks(
            place, lax.div(m, count), chips, aim_core, rows, cols, lax.rem(m, count)
        )
        f_at, s_at = (f_row, b), (s_row, b)
        if with_rows:
            a, slot = lax.div(n, slots), lax.rem(n, slots)
            base = (rows // cols) * a + lead_of(r, c, cols) + slot
            extra = jnp.where(lag_of(r, c, cols) == 0, 1, 0)
            is_row = n < lead_steps
            f_at = (jnp.where(is_row, a, f_row), jnp.where(is_row, base, b))
            s_at = (jnp.where(is_row, a, s_row), jnp.where(is_row, base + extra, b))

        def clip(at):
            return (
                jnp.clip(at[0], 0, block_rows - 1),
                jnp.clip(at[1], 0, block_cols - 1),
                0,
                0,
            )

        return clip(f_at), clip(s_at)

    def kernel(place, known_ref, schur_ref, *outs):
        n = pl.program_id(0)
        if with_rows:
            row_out, outs = outs[0], outs[1:]

            @pl.when(n < lead_steps)
            def _():
                row_out[0, 0, 0] = known_ref[0, 0].astype(jnp.bfloat16)
                row_out[0, 0, 1] = schur_ref[0, 0]

        for step, out in enumerate(outs):
            low = lead_steps + step * count

            @pl.when((n >= low) & (n < low + count))
            def _(out=out):
                out[0, 0] = known_ref[0, 0].astype(jnp.bfloat16)
                out[0, 1] = schur_ref[0, 0]

    out_specs, out_shape = [], []
    if with_rows:
        out_specs.append(
            pl.BlockSpec(
                (1, 1, 2, bs, bs),
                lambda n, place: (
                    lax.div(jnp.clip(n, 0, lead_steps - 1), slots),
                    lax.rem(jnp.clip(n, 0, lead_steps - 1), slots),
                    0,
                    0,
                    0,
                ),
            )
        )
        out_shape.append(jax.ShapeDtypeStruct((count, slots, 2, bs, bs), jnp.bfloat16))
    for step in range(chips):
        low = lead_steps + step * count
        out_specs.append(
            pl.BlockSpec(
                (1, 2, bs, bs),
                lambda n, place, low=low: (jnp.clip(n - low, 0, count - 1), 0, 0, 0),
            )
        )
        out_shape.append(jax.ShapeDtypeStruct((count, 2, bs, bs), jnp.bfloat16))
    steps = lead_steps + chips * count
    return pl.pallas_call(
        kernel,
        grid_spec=pltpu.PrefetchScalarGridSpec(
            num_scalar_prefetch=1,
            grid=(steps,),
            in_specs=[
                pl.BlockSpec((1, 1, bs, bs), lambda n, place: source(n, place)[0]),
                pl.BlockSpec((1, 1, bs, bs), lambda n, place: source(n, place)[1]),
            ],
            out_specs=out_specs,
        ),
        out_shape=out_shape,
        compiler_params=pltpu.CompilerParams(dimension_semantics=("arbitrary",)),
        cost_estimate=pl.CostEstimate(
            flops=steps * bs * bs * 200, bytes_accessed=steps * bs * bs * 10, transcendentals=0
        ),
        name="pack_rows" if with_rows else "pack_late",
    )(place, known, schur)


def copy_blocks(known):
    block_rows, block_cols, bs = known.shape[0], known.shape[1], known.shape[2]

    def kernel(source, out):
        out[...] = source[...]

    spec = pl.BlockSpec((1, block_cols, bs, bs), lambda n: (n, 0, 0, 0))
    return pl.pallas_call(
        kernel,
        grid=(block_rows,),
        in_specs=[spec],
        out_specs=spec,
        out_shape=jax.ShapeDtypeStruct(known.shape, known.dtype),
        cost_estimate=pl.CostEstimate(
            flops=known.size * 1000, bytes_accessed=known.size * 8, transcendentals=0
        ),
        name="copy_known",
    )(known)


def mm(left, right):
    return jnp.dot(left, right, preferred_element_type=jnp.float32)


def sum_base(place, row_packs, columns, own_far, row_far, col_far, late, rows, cols):
    count, slots, _, bs, _ = row_packs[0].shape
    reach = FIRST + DIAGS - 1
    far_in = [own_far] + row_far + col_far
    n_rows, n_cols, n_far = len(row_packs), len(columns), len(far_in)

    def kernel(place, *refs):
        row_in, refs = refs[:n_rows], refs[n_rows:]
        col_in, refs = refs[:n_cols], refs[n_cols:]
        far_ref, refs = refs[:n_far], refs[n_far:]
        total_out, keep_row, keep_col, row_f, row_s, col_buf, col_far_buf, total, sems = refs
        r, c = place[0], place[1]
        lag = lag_of(r, c, cols)
        is_late = (lax.rem(r, 2) == 1) & (lag == cols - 1)
        active = is_late if late else jnp.logical_not(is_late)

        @pl.when(active)
        def _():
            copies = []
            sem = 0

            def begin(src, dst):
                nonlocal sem
                copy = pltpu.make_async_copy(src, dst, sems.at[sem])
                sem += 1
                copy.start()
                return copy

            for k, ref in enumerate(row_in):
                shift = lag_of(r, jnp.bitwise_xor(c, k), cols)
                shift_s = lax.rem(shift + cols - 1, cols)
                for slot in range(slots):
                    copies.append(begin(ref.at[:, slot, 0], row_f.at[:, cols * slot + shift]))
                    copies.append(begin(ref.at[:, slot, 1], row_s.at[:, cols * slot + shift_s]))
            far_rows = []
            for g in range(1 + len(row_far)):
                src, at = far_ref[g], jnp.maximum(FIRST + lag - g - 1, FIRST)
                copy = pltpu.make_async_copy(src, row_s.at[:, at], sems.at[sem])
                sem += 1
                pl.when(lag > g)(copy.start)
                far_rows.append((g, copy))
            far_cols = []
            for g in range(1 + len(col_far)):
                src = far_ref[0] if g == 0 else far_ref[len(row_far) + g]
                far_cols.append(begin(src, col_far_buf.at[g]))
            col_copies = [begin(ref, col_buf.at[n]) for n, ref in enumerate(col_in)]
            for copy in copies:
                copy.wait()
            for g, copy in far_rows:
                pl.when(lag > g)(copy.wait)
            keep_one = begin(row_s.at[:, pl.ds(0, DIAGS - 1)], keep_row)
            for copy in far_cols:
                copy.wait()
            for a in range(count):
                part = jnp.zeros((bs, bs), jnp.float32)
                for g in range(1 + len(col_far)):
                    at = jnp.where(r + g >= rows, jnp.minimum(a + 1, count - 1), a)
                    left = row_f[a, g]
                    left = jnp.where(lag > g, left, jnp.zeros_like(left))
                    part = part + mm(left, col_far_buf[g, at])
                total[a] = part
            aim = r + lag
            for n in range(n_cols):
                step, swapped = n % (n_cols // 2), n // (n_cols // 2)
                chip = mod_add(lax.div(r, 2), step, rows // 2)
                core = lax.rem(r, 2)
                origin = 2 * chip + (1 - core if swapped else core)
                off_f = lax.rem(aim - origin + rows, rows)
                off_s = 1 + lax.rem(aim - origin - 1 + 2 * rows, rows)
                at_s = FIRST + lag - off_f - 1
                at_f = FIRST + lag - off_s
                col_copies[n].wait()
                known_there = at_f < FIRST
                for a in range(count):
                    left = row_f[a, jnp.minimum(at_f, FIRST - 1)]
                    left = jnp.where(known_there, left, jnp.zeros_like(left))
                    total[a] += mm(left, col_buf[n, a, 1]) - mm(row_s[a, at_s], col_buf[n, a, 0])

                @pl.when(off_s < DIAGS)
                def _(n=n, off_s=off_s):
                    pltpu.sync_copy(col_buf.at[n, :, 1], keep_col.at[:, off_s - 1])

            keep_one.wait()
            pltpu.sync_copy(total, total_out)

    n_sems = n_rows * slots * 2 + 1 + len(row_far) + 1 + len(col_far) + n_cols + 1
    return pl.pallas_call(
        kernel,
        in_specs=[place_spec()] + [any_spec()] * (n_rows + n_cols + n_far),
        out_specs=[any_spec()] * 3,
        out_shape=[
            jax.ShapeDtypeStruct((count, bs, bs), jnp.float32),
            jax.ShapeDtypeStruct((count, DIAGS - 1, bs, bs), jnp.bfloat16),
            jax.ShapeDtypeStruct((count, DIAGS - 1, bs, bs), jnp.bfloat16),
        ],
        scratch_shapes=[
            pltpu.VMEM((count, FIRST, bs, bs), jnp.bfloat16),
            pltpu.VMEM((count, reach, bs, bs), jnp.bfloat16),
            pltpu.VMEM((n_cols, count, 2, bs, bs), jnp.bfloat16),
            pltpu.VMEM((1 + len(col_far), count, bs, bs), jnp.bfloat16),
            pltpu.VMEM((count, bs, bs), jnp.float32),
            pltpu.SemaphoreType.DMA((n_sems,)),
        ],
        compiler_params=pltpu.CompilerParams(vmem_limit_bytes=40 * 2**20),
        cost_estimate=pl.CostEstimate(
            flops=count * 20 * 2 * bs**3, bytes_accessed=count * 40 * bs * bs * 2, transcendentals=0
        ),
        name="sum_late" if late else "sum_early",
    )(place, *row_packs, *columns, *far_in)


def halves(value):
    high = value.astype(jnp.bfloat16)
    return high, (value - high.astype(jnp.float32)).astype(jnp.bfloat16)


def solve_stage(stage, place, output, sums, late_sums, row_new, col_new, far_pairs, own_pairs, spacing, rows, cols):
    count, bs = sums[0].shape[0], sums[0].shape[1]
    block_cols = output.shape[1]
    last = stage == DIAGS - 1
    two = last and late_sums is not None
    groups = [list(sums)] + ([list(late_sums)] if two else [])
    flat = [x for group in groups for x in group]
    n_new = len(row_new)

    def kernel(place, out_in, *refs):
        group_refs, refs = refs[: len(flat)], refs[len(flat) :]
        row_in, refs = refs[:n_new], refs[n_new:]
        col_in, refs = refs[:n_new], refs[n_new:]
        pair_far, pair_own, space_in, out, sent, refs = *refs[:5], refs[5:]
        total, keep_r, keep_c, row_buf, col_buf, far_buf, own_buf, space, solved, narrow, sems = refs
        r, c = place[0], place[1]
        lag = lag_of(r, c, cols)
        is_late = (lax.rem(r, 2) == 1) & (lag == cols - 1)

        @pl.when(lag == stage)
        def _():
            sem = 0

            def plan(src, dst):
                nonlocal sem
                copy = pltpu.make_async_copy(src, dst, sems.at[sem])
                sem += 1
                return copy

            small = []
            for n in range(n_new):
                small.append(plan(row_in[n], row_buf.at[n]))
                small.append(plan(col_in[n], col_buf.at[n]))
            ours = plan(pair_own.at[pl.ds(0, count)], own_buf)
            small += [plan(pair_far, far_buf), plan(space_in, space)]
            targets = [total] + ([keep_r, keep_c] if n_new else [])
            first_sem = sem
            for at, group in enumerate([group_refs[:3], group_refs[3:]][: len(groups)]):
                chosen = is_late if at == 1 else jnp.logical_not(is_late)
                for i, dst in enumerate(targets):
                    copy = pltpu.make_async_copy(group[i], dst, sems.at[first_sem + i])
                    if two:
                        pl.when(chosen)(copy.start)
                    else:
                        copy.start()
            for copy in small + [ours]:
                copy.start()
            for i, dst in enumerate(targets):
                pltpu.make_async_copy(group_refs[i], dst, sems.at[first_sem + i]).wait()
            for copy in small + [ours]:
                copy.wait()
            lead = lead_of(r, c, cols)
            wrapped = jnp.where(r + lag >= rows, 1, 0)
            for a in range(count):
                right = total[a]
                for n in range(n_new):
                    g = stage - n
                    at = jnp.where(r + g >= rows, jnp.minimum(a + 1, count - 1), a)
                    right = right + mm(row_buf[n, a], keep_c[a, g - 1])
                    right = right - mm(keep_r[a, g - 1], col_buf[n, at])
                far = jnp.minimum(a + wrapped, count - 1)
                vec_high, vec_low = halves(own_buf[a, 0])
                inv_high, inv_low = halves(own_buf[a, 1])
                right_high, right_low = halves(right)
                mixed = mm(inv_high, right_high) + (mm(inv_high, right_low) + mm(inv_low, right_high))
                mixed_high, mixed_low = halves(mixed)
                mixed = mm(mixed_high, far_buf[far, 0]) + mm(mixed_low, far_buf[far, 0])
                mixed = mixed / space[a]
                mixed_high, mixed_low = halves(mixed)
                back = mm(vec_high, mixed_high) + (mm(vec_high, mixed_low) + mm(vec_low, mixed_high))
                back_high, back_low = halves(back)
                answer = mm(back_high, far_buf[far, 1]) + mm(back_low, far_buf[far, 1])
                solved[a] = answer
                narrow[a] = answer.astype(jnp.bfloat16)
            copies = []
            send = None
            if not last:
                send = pltpu.make_async_copy(narrow, sent, sems.at[sem])
                send.start()
            for a in range(count):
                at = (rows // cols) * a + FIRST // cols + lead
                copy = pltpu.make_async_copy(
                    solved.at[a], out.at[a, jnp.minimum(at, block_cols - 1)], sems.at[a]
                )
                pl.when(at < block_cols)(copy.start)
                copies.append((at, copy))
            for at, copy in copies:
                pl.when(at < block_cols)(copy.wait)
            if send is not None:
                send.wait()

    n_in = 1 + 1 + len(flat) + 2 * n_new + 3
    half = max(n_new, 1)
    return pl.pallas_call(
        kernel,
        in_specs=[place_spec()] + [any_spec()] * (n_in - 1),
        out_specs=[any_spec()] * 2,
        out_shape=[
            jax.ShapeDtypeStruct(output.shape, output.dtype),
            jax.ShapeDtypeStruct((count, bs, bs), jnp.bfloat16),
        ],
        input_output_aliases={1: 0},
        scratch_shapes=[
            pltpu.VMEM((count, bs, bs), jnp.float32),
            pltpu.VMEM((count, DIAGS - 1, bs, bs), jnp.bfloat16),
            pltpu.VMEM((count, DIAGS - 1, bs, bs), jnp.bfloat16),
            pltpu.VMEM((half, count, bs, bs), jnp.bfloat16),
            pltpu.VMEM((half, count, bs, bs), jnp.bfloat16),
            pltpu.VMEM((count, 2, bs, bs), jnp.bfloat16),
            pltpu.VMEM((count, 2, bs, bs), jnp.float32),
            pltpu.VMEM((count, bs, bs), jnp.float32),
            pltpu.VMEM((count, bs, bs), jnp.float32),
            pltpu.VMEM((count, bs, bs), jnp.bfloat16),
            pltpu.SemaphoreType.DMA((2 * n_new + 6 + count,)),
        ],
        compiler_params=pltpu.CompilerParams(vmem_limit_bytes=30 * 2**20),
        cost_estimate=pl.CostEstimate(
            flops=count * 12 * 2 * bs**3, bytes_accessed=count * 20 * bs * bs * 2, transcendentals=0
        ),
        name=f"solve_{stage}",
    )(place, output, *flat, *row_new, *col_new, far_pairs, own_pairs, spacing)


def banded_body(schur_blocks, known_blocks, eigen_pairs, eigenvalues):
    rows = lax.axis_size("row")
    cols = lax.axis_size("col")
    r = lax.axis_index("row")
    c = lax.axis_index("col")
    schur = schur_blocks[:, 0, :, 0]
    known = known_blocks[:, 0, :, 0]
    pairs = eigen_pairs[:, 0]
    count = known.shape[0] - 1
    block_cols = known.shape[1]
    chips = rows // 2
    devices = [(i, k) for i in range(rows) for k in range(cols)]

    def lag(i, k):
        return (k - i) % cols

    def send(block, move, keep=lambda i, k: True):
        pairs_list = []
        for i, k in devices:
            to = move(i, k)
            to = (to[0] % rows, to[1] % cols)
            if keep(*to):
                pairs_list.append((i * cols + k, to[0] * cols + to[1]))
        return lax.ppermute(block, ("row", "col"), pairs_list)

    place = jnp.stack([r, c]).astype(jnp.int32)
    packed = pack(known, schur, place, 0, rows, cols, True)
    row_pack, col_packs = packed[0], list(packed[1:])
    early = [col_packs[0]]
    row_packs = [row_pack]
    for k in range(1, cols):
        row_packs.append(send(row_pack, lambda i, j, k=k: (i, j ^ k)))
    for step in range(1, chips):
        early.append(send(col_packs[step], lambda i, j, s=step: (i - 2 * s, j)))
    early = early + [send(x, lambda i, j: (i ^ 1, j)) for x in early]

    def split_chip(i, k):
        return lag(2 * (i // 2) + 1, k) == cols - 1

    late_packs = pack(known, schur, place, 1, rows, cols, False)
    late = [late_packs[0]]
    for step in range(1, chips):
        late.append(send(late_packs[step], lambda i, j, s=step: (i - 2 * s, j), split_chip))
    late = late + [
        send(x, lambda i, j: (i ^ 1, j), lambda i, k: split_chip(i, k) and i % 2 == 1) for x in late
    ]

    lead = lead_of(r, c, cols)
    own_far = jnp.stack(
        [
            schur[a, jnp.clip((rows // cols) * a + FIRST // cols + lead, 0, block_cols - 1)]
            for a in range(count)
        ]
    )
    row_far = [
        send(own_far, lambda i, j, g=g: (i, j + g), lambda i, k, g=g: lag(i, k) > g)
        for g in range(1, DIAGS - 1)
    ]
    col_far = [
        send(own_far, lambda i, j, g=g: (i - g, j), lambda i, k, g=g: lag(i, k) > g)
        for g in range(1, DIAGS - 1)
    ]
    pair_list = [pairs[1:].astype(jnp.bfloat16)]
    for g in range(1, DIAGS):
        pair_list.append(
            send(pair_list[-1], lambda i, j: (i - 1, j), lambda i, k, g=g: lag(i, k) == g)
        )
    lag_here = lag_of(r, c, cols)
    own_ids = jnp.arange(count, dtype=jnp.int32) * rows + r
    far_ids = jnp.minimum(own_ids + FIRST + lag_here, eigenvalues.shape[0] - 1)
    spacing = eigenvalues[own_ids][:, :, None] - eigenvalues[far_ids][:, None, :]

    output = copy_blocks(known)
    sums = sum_base(place, row_packs, early, own_far, row_far, col_far, False, rows, cols)
    late_sums = sum_base(place, row_packs, late, own_far, row_far, col_far, True, rows, cols)
    row_new = {}
    col_new = {}
    for stage in range(DIAGS):
        output, fresh = solve_stage(
            stage,
            place,
            output,
            sums,
            late_sums,
            [row_new[n, stage] for n in range(stage)],
            [col_new[n, stage] for n in range(stage)],
            pair_list[stage],
            pairs,
            spacing,
            rows,
            cols,
        )
        for later in range(stage + 1, DIAGS):
            g = later - stage
            chosen = lambda i, k, later=later: lag(i, k) == later
            row_new[stage, later] = send(fresh, lambda i, j, g=g: (i, j + g), chosen)
            col_new[stage, later] = send(fresh, lambda i, j, g=g: (i - g, j), chosen)
    return output[:, None, :, None]


def solution(mesh):
    rows, cols = mesh.shape["row"], mesh.shape["col"]
    banded = rows == FIRST and cols == DIAGS
    return jax.shard_map(
        banded_body if banded else body,
        mesh=mesh,
        in_specs=(
            P(None, "row", None, "col", None, None),
            P(None, "row", None, "col", None, None),
            P(None, "row", None, None, None),
            P(),
        ),
        out_specs=P(None, "row", None, "col", None, None),
        check_vma=False,
    )
```

```python
import jax
import jax.numpy as jnp
from jax import lax
from jax.experimental import pallas as pl
from jax.experimental.pallas import tpu as pltpu
from jax.sharding import PartitionSpec as P


FIRST = 8
DIAGS = 4
VMEM_BYTES = 67_043_328


def shifted(block, axis, distance):
    devices = range(lax.axis_size(axis))
    route = [((i - distance) % len(devices), i) for i in devices]
    return lax.ppermute(block, axis, route)


def pick_rows(stacked, indices):
    return jax.vmap(lambda source, chosen: source[chosen])(stacked, indices)


def full_dot(left_side, right_side):
    return jnp.einsum(
        "apq,aqr->apr",
        left_side,
        right_side,
        precision=lax.Precision.HIGHEST,
        preferred_element_type=jnp.float32,
    )


def right_terms(known_rows, schur_rows, known_cols, schur_cols, offsets, usable, distance):
    band_width = known_rows.shape[1]
    reach_back = distance[:, :, None] - offsets
    first_mask = usable & (offsets >= 1) & (reach_back >= 0) & (reach_back <= FIRST - 1)
    second_mask = usable & (offsets <= FIRST - 1) & (reach_back >= 1)
    clipped = jnp.clip(reach_back, 0, band_width - 1)
    known_pick = jnp.where(first_mask[..., None, None], pick_rows(known_rows, clipped), 0)
    schur_pick = jnp.where(second_mask[..., None, None], -pick_rows(schur_rows, clipped), 0)
    left_side = jnp.concatenate([known_pick, schur_pick], axis=2)
    right_side = jnp.concatenate([schur_cols, known_cols], axis=2)
    return jnp.einsum(
        "atepq,ateqr->atpr", left_side, right_side, preferred_element_type=jnp.float32
    )


def body(schur_blocks, known_blocks, eigen_pairs, eigenvalues):
    row_count = lax.axis_size("row")
    col_count = lax.axis_size("col")
    row_index = lax.axis_index("row")
    col_index = lax.axis_index("col")
    schur_local = schur_blocks[:, 0, :, 0]
    known_local = known_blocks[:, 0, :, 0]
    pairs_local = eigen_pairs[:, 0]
    block_rows = schur_local.shape[0]
    block_cols = schur_local.shape[1]
    blocks_total = block_rows * row_count
    band_width = FIRST + DIAGS
    row_slots = -(-band_width // col_count)
    col_slots = -(-band_width // row_count)
    per_row = -(-DIAGS // col_count)
    row_ids = jnp.arange(block_rows, dtype=jnp.int32) * row_count + row_index
    col_ids = jnp.arange(block_cols, dtype=jnp.int32) * col_count + col_index
    band_range = jnp.arange(band_width, dtype=jnp.int32)
    row_range = jnp.arange(block_rows, dtype=jnp.int32)
    row_offsets = (
        jnp.mod(col_index - row_ids, col_count)[:, None]
        + jnp.arange(row_slots, dtype=jnp.int32)[None, :] * col_count
    )
    row_reach = row_ids[:, None] + row_offsets
    row_valid = (row_offsets < band_width) & (row_reach < blocks_total)
    row_pick = jnp.clip(row_reach // col_count, 0, block_cols - 1)
    known_send = jnp.where(
        row_valid[..., None, None], pick_rows(known_local, row_pick), 0.0
    ).astype(jnp.bfloat16)
    schur_send = jnp.where(row_valid[..., None, None], pick_rows(schur_local, row_pick), 0)
    known_recv, schur_recv = (
        lax.all_gather(known_send[None], "col", axis=0, tiled=True),
        lax.all_gather(schur_send[None], "col", axis=0, tiled=True),
    )
    row_source = jnp.mod(row_ids[:, None] + band_range[None, :], col_count)
    row_slot = (band_range // col_count)[None, :]
    known_rows = known_recv[row_source, row_range[:, None], row_slot]
    schur_rows = schur_recv[row_source, row_range[:, None], row_slot]
    col_offsets = (
        jnp.mod(col_ids - row_index, row_count)[:, None]
        + jnp.arange(col_slots, dtype=jnp.int32)[None, :] * row_count
    )
    col_reach = col_ids[:, None] - col_offsets
    col_valid = (col_offsets < band_width) & (col_reach >= 0)
    col_pick = jnp.clip(col_reach // row_count, 0, block_rows - 1)
    known_down = jnp.where(
        col_valid[..., None, None], pick_rows(jnp.swapaxes(known_local, 0, 1), col_pick), 0.0
    ).astype(jnp.bfloat16)
    schur_down = jnp.where(
        col_valid[..., None, None], pick_rows(jnp.swapaxes(schur_local, 0, 1), col_pick), 0
    )
    target_first = -((col_index - row_ids - FIRST) // col_count)
    target_block = target_first[:, None] + jnp.arange(per_row, dtype=jnp.int32)[None, :]
    target_cols = target_block * col_count + col_index
    distance = target_cols - row_ids[:, None]
    active = (target_block < block_cols) & (distance <= FIRST + DIAGS - 1)
    target_clip = jnp.clip(target_block, 0, block_cols - 1)
    own_strip = jnp.stack([known_down, schur_down])
    collected = jnp.zeros((row_count,) + own_strip.shape, jnp.bfloat16)
    collected = collected.at[row_index].set(own_strip)
    reach_rows = min(row_count, band_width)
    carried = own_strip
    for step in range(1, reach_rows):
        carried = shifted(carried, "row", row_count - 1)
        collected = collected.at[jnp.mod(row_index + step, row_count)].set(carried)
    known_all = collected[:, 0]
    schur_all = collected[:, 1]
    col_source = jnp.mod(target_cols[:, :, None] - band_range[None, None, :], row_count)
    col_slot = (band_range // row_count)[None, None, :]
    known_cols = known_all[col_source, target_clip[:, :, None], col_slot]
    schur_cols = schur_all[col_source, target_clip[:, :, None], col_slot]
    offsets = jnp.broadcast_to(band_range[None, None, :], col_source.shape)
    totals = right_terms(
        known_rows,
        schur_rows,
        known_cols,
        schur_cols,
        offsets,
        jnp.ones(offsets.shape, jnp.bool_),
        distance,
    )
    kept_cols = schur_cols[:, :, :DIAGS]
    pair_list = []
    for distance_now in range(FIRST, FIRST + DIAGS):
        lag = distance_now % row_count
        receiver = jnp.mod(row_index - lag, row_count)
        wanted = jnp.clip(
            (row_range * row_count + receiver + distance_now) // row_count, 0, block_rows - 1
        )
        sending = pairs_local[wanted]
        if lag == 0:
            pair_list.append(sending)
        else:
            pair_list.append(
                shifted(sending.astype(jnp.bfloat16), "row", row_count - lag).astype(sending.dtype)
            )
    vec_left = pairs_local[:, 0]
    inv_left = pairs_local[:, 1]
    lam_left = eigenvalues[row_ids]
    output = known_local
    for distance_now in range(FIRST, FIRST + DIAGS):
        hitting = active & (distance == distance_now)
        solving = jnp.any(hitting, axis=1)
        chosen = jnp.sum(jnp.where(hitting[..., None, None], totals, 0.0), axis=1)
        block_col = jnp.sum(jnp.where(hitting, target_clip, 0), axis=1)
        block_ids = jnp.clip(block_col * col_count + col_index, 0, blocks_total - 1)
        vec_right = pair_list[distance_now - FIRST][:, 0]
        inv_right = pair_list[distance_now - FIRST][:, 1]
        lam_right = eigenvalues[block_ids]
        spacing = lam_left[:, :, None] - lam_right[:, None, :]
        spacing = jnp.where(solving[:, None, None], spacing, 1.0)
        mixed_block = full_dot(full_dot(inv_left, chosen), vec_right) / spacing
        solved = full_dot(full_dot(vec_left, mixed_block), inv_right)
        solved = jnp.where(solving[:, None, None], solved, 0.0)
        placing = solving[:, None] & (
            jnp.arange(block_cols, dtype=jnp.int32)[None, :] == block_col[:, None]
        )
        output = jnp.where(placing[:, :, None, None], solved[:, None], output)
        if distance_now < FIRST + DIAGS - 1:
            rounded = solved.astype(jnp.bfloat16)
            for gap in range(1, FIRST + DIAGS - distance_now):
                row_new = shifted(rounded, "col", gap)
                receiver = jnp.mod(row_index - gap, row_count)
                wanted = jnp.clip(
                    (row_range * row_count + receiver + gap) // row_count, 0, block_rows - 1
                )
                col_new = shifted(rounded[wanted], "row", row_count - gap)
                growing = active & (distance - distance_now == gap)
                known_from_row = row_new[:, None]
                known_from_col = col_new[:, None]
                schur_from_row = schur_rows[:, gap][:, None]
                schur_from_col = kept_cols[:, :, gap]
                left_side = jnp.stack(
                    [
                        jnp.where(growing[..., None, None], known_from_row, 0),
                        jnp.where(growing[..., None, None], -schur_from_row, 0),
                    ],
                    axis=2,
                )
                right_side = jnp.stack([schur_from_col, known_from_col], axis=2)
                totals = totals + jnp.einsum(
                    "atepq,ateqr->atpr", left_side, right_side, preferred_element_type=jnp.float32
                )
    return output[:, None, :, None]


ROUNDS = {0: [[(0, 1)]], 1: [[(1, 2), (0, 3)], [(0, 2), (1, 3)]], 2: [[(2, 3)]]}


def lag_of(r, c, cols):
    return lax.rem(c - r + 2 * cols * FIRST, cols)


def lead_of(r, c, cols):
    return lax.div(r - c + lag_of(r, c, cols), cols)


def any_spec():
    return pl.BlockSpec(memory_space=pltpu.HBM)


def place_spec():
    return pl.BlockSpec(memory_space=pltpu.SMEM)


def mod_add(value, shift, size):
    return lax.rem(value + shift + 4 * size, size)


def mirrored(step, c, cols):
    return jnp.where(c >= cols // 2, -step, step)


def column_picks(place, step, chips, aim_core, rows, cols, a):
    r, c = place[0], place[1]
    chip = mod_add(lax.div(r, 2), -step, chips)
    lead = lead_of(2 * chip + aim_core, c, cols)
    j = rows * a + FIRST + cols * lead + c
    off_f = lax.rem(j - r + rows, rows)
    off_s = 1 + lax.rem(j - r - 1 + rows, rows)
    return lax.div(j - off_f - r, rows), lax.div(j - off_s - r, rows), (j - c) // cols


def pack(known, schur, place, aim_core, rows, cols, first):
    block_rows, block_cols, bs = known.shape[0], known.shape[1], known.shape[2]
    count = block_rows - 1
    chips = rows // 2
    slots = FIRST // cols

    n_rows = slots if first else 0
    shapes = [(count, 2, bs, bs)] * (n_rows + chips) + ([(count, bs, bs)] if first else [])
    total = count * (n_rows + chips)

    def kernel(place, known_ref, schur_ref, *refs):
        outs, refs = refs[: len(shapes)], refs[len(shapes) :]
        bufs, refs = refs[: len(shapes)], refs[len(shapes) :]
        wide, in_sems, out_sems, far_sems = refs
        r, c = place[0], place[1]
        lead = lead_of(r, c, cols)
        groups = []
        for step in [chips // 2] + [x for x in range(1, chips) if x != chips // 2] + [0]:
            picks = []
            for a in range(count):
                way = step if first else mirrored(step, c, cols)
                f_row, s_row, b = column_picks(place, way, chips, aim_core, rows, cols, a)
                picks.append(((f_row, b), (s_row, b)))
            groups.append((n_rows + step, picks))
        extra = jnp.where(lag_of(r, c, cols) == 0, 1, 0)
        for slot in range(n_rows):
            picks = []
            for a in range(count):
                base = (rows // cols) * a + lead + slot
                picks.append(((a, base), (a, base + extra)))
            groups.insert(1 + slot, (slot, picks))

        def clip(at):
            return jnp.clip(at[0], 0, block_rows - 1), jnp.clip(at[1], 0, block_cols - 1)

        n = 0
        plans = []
        for at, picks in groups:
            mine = []
            for a, (f_at, s_at) in enumerate(picks):
                f_at, s_at = clip(f_at), clip(s_at)
                low = pltpu.make_async_copy(known_ref.at[f_at[0], f_at[1]], wide.at[n], in_sems.at[n, 0])
                thin = pltpu.make_async_copy(
                    schur_ref.at[s_at[0], s_at[1]], bufs[at].at[a, 1], in_sems.at[n, 1]
                )
                low.start()
                thin.start()
                mine.append((n, low, thin, a))
                n += 1
            plans.append((at, mine))
        fars = []
        if first:
            for a in range(count):
                at = clip((a, (rows // cols) * a + FIRST // cols + lead))
                far = pltpu.make_async_copy(schur_ref.at[at[0], at[1]], bufs[-1].at[a], far_sems.at[a])
                far.start()
                fars.append(far)
        sends = []
        for at, mine in plans:
            for n, low, thin, a in mine:
                low.wait()
                bufs[at][a, 0] = wide[n].astype(jnp.bfloat16)
                thin.wait()
            out = pltpu.make_async_copy(bufs[at], outs[at], out_sems.at[at])
            out.start()
            sends.append(out)
        if first:
            for far in fars:
                far.wait()
            out = pltpu.make_async_copy(bufs[-1], outs[-1], out_sems.at[len(shapes) - 1])
            out.start()
            sends.append(out)
        for out in sends:
            out.wait()

    return pl.pallas_call(
        kernel,
        in_specs=[place_spec(), any_spec(), any_spec()],
        out_specs=[any_spec()] * len(shapes),
        out_shape=[jax.ShapeDtypeStruct(x, jnp.bfloat16) for x in shapes],
        scratch_shapes=[pltpu.VMEM(x, jnp.bfloat16) for x in shapes]
        + [
            pltpu.VMEM((total, bs, bs), jnp.float32),
            pltpu.SemaphoreType.DMA((total, 2)),
            pltpu.SemaphoreType.DMA((len(shapes),)),
            pltpu.SemaphoreType.DMA((count,)),
        ],
        compiler_params=pltpu.CompilerParams(vmem_limit_bytes=VMEM_BYTES),
        cost_estimate=pl.CostEstimate(
            flops=total * bs * bs * 200, bytes_accessed=total * bs * bs * 10, transcendentals=0
        ),
        name="pack_first" if first else "pack_late",
    )(place, known, schur)


def copy_blocks(known):
    block_rows, block_cols, bs = known.shape[0], known.shape[1], known.shape[2]

    def kernel(source, out):
        out[...] = source[...]

    spec = pl.BlockSpec((1, block_cols, bs, bs), lambda n: (n, 0, 0, 0))
    return pl.pallas_call(
        kernel,
        grid=(block_rows,),
        in_specs=[spec],
        out_specs=spec,
        out_shape=jax.ShapeDtypeStruct(known.shape, known.dtype),
        compiler_params=pltpu.CompilerParams(vmem_limit_bytes=VMEM_BYTES),
        cost_estimate=pl.CostEstimate(
            flops=known.size * 1000, bytes_accessed=known.size * 8, transcendentals=0
        ),
        name="copy_known",
    )(known)


def mm(left, right):
    return jnp.dot(left, right, preferred_element_type=jnp.float32)


def own_lag(place, cols):
    r, c = place[0], place[1]
    lag = lag_of(r, c, cols)
    return r, c, lag, (lax.rem(r, 2) == 1) & (lag == cols - 1)


def offsets_of(r, lag, step, crossed, rows):
    chip = mod_add(lax.div(r, 2), step, rows // 2)
    core = lax.rem(r, 2)
    origin = 2 * chip + (1 - core if crossed else core)
    aim = r + lag
    return lax.rem(aim - origin + rows, rows), 1 + lax.rem(aim - origin - 1 + 2 * rows, rows)


def sum_base(place, row_parts, columns, after, own_far, row_far, col_far, late, rows, cols):
    count, _, bs, _ = row_parts[0][0].shape
    slots = len(row_parts[0])
    reach = FIRST + DIAGS - 1
    far_in = [own_far] + row_far + col_far
    flat_rows = [x for parts in row_parts for x in parts]
    n_rows, n_cols, n_far, n_after = len(flat_rows), len(columns), len(far_in), len(after)

    def kernel(place, *refs):
        row_in, refs = refs[:n_rows], refs[n_rows:]
        col_in, refs = refs[:n_cols], refs[n_cols:]
        far_ref, refs = refs[:n_far], refs[n_far:]
        outs, refs = refs[: 3 + (1 if n_after else 0)], refs[3 + (1 if n_after else 0) :]
        total_out, keep_row, keep_col = outs[:3]
        row_f, row_s, col_buf, col_far_buf, left_buf, total, sems = refs
        r, c, lag, is_late = own_lag(place, cols)
        active = is_late if late else jnp.logical_not(is_late)

        @pl.when(active)
        def _():
            sem = 0

            def plan(src, dst):
                nonlocal sem
                copy = pltpu.make_async_copy(src, dst, sems.at[sem])
                sem += 1
                return copy

            def begin(src, dst):
                copy = plan(src, dst)
                copy.start()
                return copy

            copies = []
            for n, ref in enumerate(row_in):
                shift = lag_of(r, jnp.bitwise_xor(c, n // slots), cols)
                shift_s = lax.rem(shift + cols - 1, cols)
                slot = n % slots
                copies.append(begin(ref.at[:, 0], row_f.at[:, cols * slot + shift]))
                copies.append(begin(ref.at[:, 1], row_s.at[:, cols * slot + shift_s]))
            far_rows = []
            for g in range(1 + len(row_far)):
                copy = plan(far_ref[g], row_s.at[:, jnp.maximum(FIRST + lag - g - 1, FIRST)])
                pl.when(lag > g)(copy.start)
                far_rows.append((g, copy))
            for g in range(1 + len(col_far)):
                src = far_ref[0] if g == 0 else far_ref[len(row_far) + g]
                copies.append(begin(src, col_far_buf.at[g]))
            col_copies = [begin(ref, col_buf.at[n]) for n, ref in enumerate(col_in)]
            for copy in copies:
                copy.wait()
            for g, copy in far_rows:
                pl.when(lag > g)(copy.wait)
            keeps = [(None, begin(row_s.at[:, pl.ds(0, DIAGS - 1)], keep_row))]

            def lefts(step, crossed, a):
                way = mirrored(step, c, cols) if late else step
                off_f, off_s = offsets_of(r, lag, way, crossed, rows)
                at_f = FIRST + lag - off_s
                left = row_f[a, jnp.minimum(at_f, FIRST - 1)]
                left = jnp.where(at_f < FIRST, left, jnp.zeros_like(left))
                return left, row_s[a, FIRST + lag - off_f - 1]

            for n, (step, crossed) in enumerate(after):
                for a in range(count):
                    left_buf[a, 2 * n], left_buf[a, 2 * n + 1] = lefts(step, crossed, a)
            if n_after:
                keeps.append((None, begin(left_buf, outs[3])))
            for a in range(count):
                part = jnp.zeros((bs, bs), jnp.float32)
                for g in range(1 + len(col_far)):
                    at = jnp.where(r + g >= rows, jnp.minimum(a + 1, count - 1), a)
                    left = row_f[a, g]
                    left = jnp.where(lag > g, left, jnp.zeros_like(left))
                    part = part + mm(left, col_far_buf[g, at])
                total[a] = part
            for n, (_, step, crossed) in enumerate(columns):
                way = mirrored(step, c, cols) if late else step
                off_s = offsets_of(r, lag, way, crossed, rows)[1]
                col_copies[n].wait()
                for a in range(count):
                    with_s, with_f = lefts(step, crossed, a)
                    total[a] += mm(with_s, col_buf[n, a, 1]) - mm(with_f, col_buf[n, a, 0])
                save = plan(col_buf.at[n, :, 1], keep_col.at[:, jnp.minimum(off_s, DIAGS - 1) - 1])
                pl.when(off_s < DIAGS)(save.start)
                keeps.append((off_s, save))
            out = begin(total, total_out)
            for off_s, copy in keeps:
                if off_s is None:
                    copy.wait()
                else:
                    pl.when(off_s < DIAGS)(copy.wait)
            out.wait()

    out_shape = [
        jax.ShapeDtypeStruct((count, bs, bs), jnp.float32),
        jax.ShapeDtypeStruct((count, DIAGS - 1, bs, bs), jnp.bfloat16),
        jax.ShapeDtypeStruct((count, DIAGS - 1, bs, bs), jnp.bfloat16),
    ]
    if n_after:
        out_shape.append(jax.ShapeDtypeStruct((count, 2 * n_after, bs, bs), jnp.bfloat16))
    return pl.pallas_call(
        kernel,
        in_specs=[place_spec()] + [any_spec()] * (n_rows + n_cols + n_far),
        out_specs=[any_spec()] * len(out_shape),
        out_shape=out_shape,
        scratch_shapes=[
            pltpu.VMEM((count, FIRST, bs, bs), jnp.bfloat16),
            pltpu.VMEM((count, reach, bs, bs), jnp.bfloat16),
            pltpu.VMEM((n_cols, count, 2, bs, bs), jnp.bfloat16),
            pltpu.VMEM((1 + len(col_far), count, bs, bs), jnp.bfloat16),
            pltpu.VMEM((count, max(2 * n_after, 1), bs, bs), jnp.bfloat16),
            pltpu.VMEM((count, bs, bs), jnp.float32),
            pltpu.SemaphoreType.DMA((2 * n_rows + n_far + 2 * n_cols + 4,)),
        ],
        compiler_params=pltpu.CompilerParams(vmem_limit_bytes=VMEM_BYTES),
        cost_estimate=pl.CostEstimate(
            flops=count * 18 * 2 * bs**3, bytes_accessed=count * 40 * bs * bs * 2, transcendentals=0
        ),
        name="sum_late" if late else "sum_early",
    )(place, *flat_rows, *[x for x, _, _ in columns], *far_in)


def sum_rest(place, columns, sums, late, rows, cols):
    total_in, keep_row, keep_col, lefts = sums
    count, bs = total_in.shape[0], total_in.shape[1]
    n_cols = len(columns)

    def kernel(place, *refs):
        col_in, refs = refs[:n_cols], refs[n_cols:]
        old, _, left_in, total_out, keep_out, col_buf, left_buf, total, sems = refs
        r, c, lag, is_late = own_lag(place, cols)

        @pl.when(is_late if late else jnp.logical_not(is_late))
        def _():
            copies = [pltpu.make_async_copy(old, total, sems.at[0])]
            copies.append(pltpu.make_async_copy(left_in, left_buf, sems.at[1]))
            for n, ref in enumerate(col_in):
                copies.append(pltpu.make_async_copy(ref, col_buf.at[n], sems.at[2 + n]))
            for copy in copies:
                copy.start()
            for copy in copies:
                copy.wait()
            saves = []
            for n, (_, step, crossed) in enumerate(columns):
                way = mirrored(step, c, cols) if late else step
                off_s = offsets_of(r, lag, way, crossed, rows)[1]
                save = pltpu.make_async_copy(
                    col_buf.at[n, :, 1],
                    keep_out.at[:, jnp.minimum(off_s, DIAGS - 1) - 1],
                    sems.at[2 + n],
                )
                pl.when(off_s < DIAGS)(save.start)
                saves.append((off_s, save))
            for a in range(count):
                part = total[a]
                for n in range(n_cols):
                    part = part + mm(left_buf[a, 2 * n], col_buf[n, a, 1])
                    part = part - mm(left_buf[a, 2 * n + 1], col_buf[n, a, 0])
                total[a] = part
            out = pltpu.make_async_copy(total, total_out, sems.at[0])
            out.start()
            for off_s, save in saves:
                pl.when(off_s < DIAGS)(save.wait)
            out.wait()

    first = 1 + n_cols
    total, keep_col = pl.pallas_call(
        kernel,
        in_specs=[place_spec()] + [any_spec()] * (n_cols + 3),
        out_specs=[any_spec()] * 2,
        out_shape=[
            jax.ShapeDtypeStruct(total_in.shape, total_in.dtype),
            jax.ShapeDtypeStruct(keep_col.shape, keep_col.dtype),
        ],
        input_output_aliases={first: 0, first + 1: 1},
        scratch_shapes=[
            pltpu.VMEM((n_cols, count, 2, bs, bs), jnp.bfloat16),
            pltpu.VMEM(lefts.shape, jnp.bfloat16),
            pltpu.VMEM((count, bs, bs), jnp.float32),
            pltpu.SemaphoreType.DMA((2 + n_cols,)),
        ],
        compiler_params=pltpu.CompilerParams(vmem_limit_bytes=VMEM_BYTES),
        cost_estimate=pl.CostEstimate(
            flops=count * 4 * 2 * bs**3, bytes_accessed=count * 12 * bs * bs * 2, transcendentals=0
        ),
        name="rest_late" if late else "sum_rest",
    )(place, *[x for x, _, _ in columns], total_in, keep_col, lefts)
    return total, keep_row, keep_col


def halves(value):
    high = value.astype(jnp.bfloat16)
    return high, (value - high.astype(jnp.float32)).astype(jnp.bfloat16)


def solve_stage(
    stage, place, output, carried, sums, late_sums, row_new, col_new, far_pairs, own_pairs, spacing, rows, cols
):
    count, bs = sums[0].shape[0], sums[0].shape[1]
    block_cols = output.shape[1]
    last = stage == DIAGS - 1
    two = last and late_sums is not None
    groups = [list(sums)] + ([list(late_sums)] if two else [])
    flat = [x for group in groups for x in group]
    n_new = len(row_new)

    passed = [] if carried is None else [carried]

    def kernel(place, out_in, *refs):
        refs = refs[len(passed) :]
        group_refs, refs = refs[: len(flat)], refs[len(flat) :]
        row_in, refs = refs[:n_new], refs[n_new:]
        col_in, refs = refs[:n_new], refs[n_new:]
        pair_far, pair_own, space_in, out, sent, refs = *refs[:5], refs[5:]
        total, keep_r, keep_c, row_buf, col_buf, far_buf, own_buf, space, solved, narrow, sems = refs
        r, c = place[0], place[1]
        lag = lag_of(r, c, cols)
        is_late = (lax.rem(r, 2) == 1) & (lag == cols - 1)

        @pl.when(lag == stage)
        def _():
            sem = 0

            def plan(src, dst):
                nonlocal sem
                copy = pltpu.make_async_copy(src, dst, sems.at[sem])
                sem += 1
                return copy

            small = []
            for n in range(n_new):
                small.append(plan(row_in[n], row_buf.at[n]))
                small.append(plan(col_in[n], col_buf.at[n]))
            ours = plan(pair_own.at[pl.ds(0, count)], own_buf)
            small += [plan(pair_far, far_buf), plan(space_in, space)]
            targets = [total] + ([keep_r, keep_c] if n_new else [])
            first_sem = sem
            for at, group in enumerate([group_refs[:3], group_refs[3:]][: len(groups)]):
                chosen = is_late if at == 1 else jnp.logical_not(is_late)
                for i, dst in enumerate(targets):
                    copy = pltpu.make_async_copy(group[i], dst, sems.at[first_sem + i])
                    if two:
                        pl.when(chosen)(copy.start)
                    else:
                        copy.start()
            for copy in small + [ours]:
                copy.start()
            for i, dst in enumerate(targets):
                pltpu.make_async_copy(group_refs[i], dst, sems.at[first_sem + i]).wait()
            for copy in small + [ours]:
                copy.wait()
            lead = lead_of(r, c, cols)
            wrapped = jnp.where(r + lag >= rows, 1, 0)
            each = range(count)
            right = [total[a] for a in each]
            for n in range(n_new):
                g = stage - n
                for a in each:
                    at = jnp.where(r + g >= rows, jnp.minimum(a + 1, count - 1), a)
                    right[a] = right[a] + mm(row_buf[n, a], keep_c[a, g - 1])
                    right[a] = right[a] - mm(keep_r[a, g - 1], col_buf[n, at])
            far = [jnp.minimum(a + wrapped, count - 1) for a in each]

            def from_left(side, values):
                left = [halves(own_buf[a, side]) for a in each]
                value = [halves(x) for x in values]
                return [
                    mm(left[a][0], value[a][0])
                    + (mm(left[a][0], value[a][1]) + mm(left[a][1], value[a][0]))
                    for a in each
                ]

            def from_right(values, side):
                value = [halves(x) for x in values]
                return [
                    mm(value[a][0], far_buf[far[a], side]) + mm(value[a][1], far_buf[far[a], side])
                    for a in each
                ]

            mixed = from_right(from_left(1, right), 0)
            mixed = [mixed[a] / space[a] for a in each]
            answer = from_right(from_left(0, mixed), 1)
            for a in each:
                narrow[a] = answer[a].astype(jnp.bfloat16)
                solved[a] = answer[a]
            copies = []
            send = None
            if not last:
                send = pltpu.make_async_copy(narrow, sent, sems.at[sem])
                send.start()
            for a in range(count):
                at = (rows // cols) * a + FIRST // cols + lead
                copy = pltpu.make_async_copy(
                    solved.at[a], out.at[a, jnp.minimum(at, block_cols - 1)], sems.at[a]
                )
                pl.when(at < block_cols)(copy.start)
                copies.append((at, copy))
            for at, copy in copies:
                pl.when(at < block_cols)(copy.wait)
            if send is not None:
                send.wait()

    n_in = 2 + len(passed) + len(flat) + 2 * n_new + 3
    half = max(n_new, 1)
    return pl.pallas_call(
        kernel,
        in_specs=[place_spec()] + [any_spec()] * (n_in - 1),
        out_specs=[any_spec()] * 2,
        out_shape=[
            jax.ShapeDtypeStruct(output.shape, output.dtype),
            jax.ShapeDtypeStruct((count, bs, bs), jnp.bfloat16),
        ],
        input_output_aliases={1 + i: i for i in range(1 + len(passed))},
        scratch_shapes=[
            pltpu.VMEM((count, bs, bs), jnp.float32),
            pltpu.VMEM((count, DIAGS - 1, bs, bs), jnp.bfloat16),
            pltpu.VMEM((count, DIAGS - 1, bs, bs), jnp.bfloat16),
            pltpu.VMEM((half, count, bs, bs), jnp.bfloat16),
            pltpu.VMEM((half, count, bs, bs), jnp.bfloat16),
            pltpu.VMEM((count, 2, bs, bs), jnp.bfloat16),
            pltpu.VMEM((count, 2, bs, bs), jnp.float32),
            pltpu.VMEM((count, bs, bs), jnp.float32),
            pltpu.VMEM((count, bs, bs), jnp.float32),
            pltpu.VMEM((count, bs, bs), jnp.bfloat16),
            pltpu.SemaphoreType.DMA((2 * n_new + 6 + count,)),
        ],
        compiler_params=pltpu.CompilerParams(vmem_limit_bytes=VMEM_BYTES),
        cost_estimate=pl.CostEstimate(
            flops=count * 12 * 2 * bs**3, bytes_accessed=count * 20 * bs * bs * 2, transcendentals=0
        ),
    )(place, output, *passed, *flat, *row_new, *col_new, far_pairs, own_pairs, spacing)


def banded_body(schur_blocks, known_blocks, eigen_pairs, eigenvalues):
    return banded_steps(schur_blocks, known_blocks, eigen_pairs, eigenvalues)


def banded_steps(schur_blocks, known_blocks, eigen_pairs, eigenvalues):
    rows = lax.axis_size("row")
    cols = lax.axis_size("col")
    r = lax.axis_index("row")
    c = lax.axis_index("col")
    schur = schur_blocks[:, 0, :, 0]
    known = known_blocks[:, 0, :, 0]
    pairs = eigen_pairs[:, 0]
    count = known.shape[0] - 1
    chips = rows // 2
    slots = FIRST // cols
    devices = [(i, k) for i in range(rows) for k in range(cols)]

    def lag(i, k):
        return (k - i) % cols

    def send(block, move, keep=lambda i, k: True, senders=None):
        routes = []
        for i, k in devices:
            if senders is not None and lag(i, k) not in senders:
                continue
            to = move(i, k)
            to = (to[0] % rows, to[1] % cols)
            if keep(*to):
                routes.append((i * cols + k, to[0] * cols + to[1]))
        return lax.ppermute(block, ("row", "col"), routes)

    def late_core(i, k):
        return lag(i, k) == cols - 1 and i % 2 == 1

    place = jnp.stack([r, c]).astype(jnp.int32)
    packed = pack(known, schur, place, 0, rows, cols, True)
    own_parts, col_packs, own_far = packed[:slots], packed[slots:-1], packed[-1]
    early = {0: col_packs[0]}
    for step in range(1, chips):
        early[step] = send(col_packs[step], lambda i, j, s=step: (i - 2 * s, j))
    row_parts = [list(own_parts)]
    for k in (1, 2):
        row_parts.append([send(part, lambda i, j, k=k: (i, j ^ k)) for part in own_parts])
    row_parts.append(
        [
            send(row_parts[1][0], lambda i, j: (i, j ^ 2)),
            send(row_parts[2][1], lambda i, j: (i, j ^ 1)),
        ]
    )
    row_far, col_far = [], []
    for g in range(1, DIAGS - 1):
        takes = lambda i, k, g=g: lag(i, k) > g
        row_far.append(send(own_far, lambda i, j, g=g: (i, j + g), takes))
        col_far.append(send(own_far, lambda i, j, g=g: (i - g, j), takes))
    pair_list = [lax.optimization_barrier((pairs, own_far))[0][1:].astype(jnp.bfloat16)]
    for g in range(1, DIAGS):
        takes = lambda i, k, g=g: lag(i, k) == g
        pair_list.append(send(pair_list[-1], lambda i, j: (i - 1, j), takes))
    lag_here = lag_of(r, c, cols)
    own_ids = jnp.arange(count, dtype=jnp.int32) * rows + r
    far_ids = jnp.minimum(own_ids + FIRST + lag_here, eigenvalues.shape[0] - 1)
    spacing = eigenvalues[own_ids][:, :, None] - eigenvalues[far_ids][:, None, :]
    spacing = lax.optimization_barrier((spacing, own_far))[0]
    late_packs = pack(known, schur, place, 1, rows, cols, False)
    output = copy_blocks(known)

    crossed = {n: send(early[n], lambda i, j: (i ^ 1, j)) for n in range(chips)}
    late = [(late_packs[0], 0, False)]
    late_last = []
    for step in range(chips):

        def onward(i, j, step=step):
            return i - 2 * (step if j < cols // 2 else -step), j

        def onward_across(i, j, onward=onward):
            return onward(i, j)[0] ^ 1, j

        into = late_last if step == chips // 2 else late
        if step:
            into.append((send(late_packs[step], onward, late_core), step, False))
        into.append((send(late_packs[step], onward_across, late_core), step, True))
    final = chips // 2
    last = [(early[final], final, False), (crossed[final], final, True)]
    ready = []
    for step in range(chips):
        if step != final:
            ready += [(early[step], step, False), (crossed[step], step, True)]
    sums = sum_base(
        place, row_parts, ready, [x[1:] for x in last], own_far, row_far, col_far, False, rows, cols
    )
    sums = sum_rest(place, last, sums, False, rows, cols)
    late_sums = sum_base(
        place, row_parts, late, [x[1:] for x in late_last], own_far, row_far, col_far, True, rows, cols
    )
    late_sums = sum_rest(place, late_last, late_sums, True, rows, cols)
    carried = None
    row_new = {}
    col_new = {}
    for stage in range(DIAGS):
        output, carried = solve_stage(
            stage,
            place,
            output,
            carried,
            sums,
            late_sums,
            [row_new[n, stage] for n in range(stage)],
            [col_new[n, stage] for n in range(stage)],
            pair_list[stage],
            pairs,
            spacing,
            rows,
            cols,
        )
        for hops in ROUNDS.get(stage, ()):
            by_lag = dict(hops)
            takes = set(by_lag.values())

            def gap(i, k):
                return by_lag.get(lag(i, k), lag(i, k)) - lag(i, k)

            def wanted(i, k):
                return lag(i, k) in takes

            across = send(carried, lambda i, j: (i, j + gap(i, j)), wanted, by_lag)
            upward = send(carried, lambda i, j: (i - gap(i, j), j), wanted, by_lag)
            for hop in hops:
                row_new[hop] = across
                col_new[hop] = upward
    return output[:, None, :, None]


def solution(mesh):
    rows, cols = mesh.shape["row"], mesh.shape["col"]
    banded = rows == FIRST and cols == DIAGS
    return jax.shard_map(
        banded_body if banded else body,
        mesh=mesh,
        in_specs=(
            P(None, "row", None, "col", None, None),
            P(None, "row", None, "col", None, None),
            P(None, "row", None, None, None),
            P(),
        ),
        out_specs=P(None, "row", None, "col", None, None),
        check_vma=False,
    )
```

```python
import jax
import jax.numpy as jnp
from jax import lax
from jax.experimental import pallas as pl
from jax.experimental.pallas import tpu as pltpu
from jax.sharding import PartitionSpec as P


FIRST = 8
DIAGS = 4
VMEM_BYTES = 67_043_328


def shifted(block, axis, distance):
    devices = range(lax.axis_size(axis))
    route = [((i - distance) % len(devices), i) for i in devices]
    return lax.ppermute(block, axis, route)


def pick_rows(stacked, indices):
    return jax.vmap(lambda source, chosen: source[chosen])(stacked, indices)


def full_dot(left_side, right_side):
    return jnp.einsum(
        "apq,aqr->apr",
        left_side,
        right_side,
        precision=lax.Precision.HIGHEST,
        preferred_element_type=jnp.float32,
    )


def right_terms(known_rows, schur_rows, known_cols, schur_cols, offsets, usable, distance):
    band_width = known_rows.shape[1]
    reach_back = distance[:, :, None] - offsets
    first_mask = usable & (offsets >= 1) & (reach_back >= 0) & (reach_back <= FIRST - 1)
    second_mask = usable & (offsets <= FIRST - 1) & (reach_back >= 1)
    clipped = jnp.clip(reach_back, 0, band_width - 1)
    known_pick = jnp.where(first_mask[..., None, None], pick_rows(known_rows, clipped), 0)
    schur_pick = jnp.where(second_mask[..., None, None], -pick_rows(schur_rows, clipped), 0)
    left_side = jnp.concatenate([known_pick, schur_pick], axis=2)
    right_side = jnp.concatenate([schur_cols, known_cols], axis=2)
    return jnp.einsum(
        "atepq,ateqr->atpr", left_side, right_side, preferred_element_type=jnp.float32
    )


def body(schur_blocks, known_blocks, eigen_pairs, eigenvalues):
    row_count = lax.axis_size("row")
    col_count = lax.axis_size("col")
    row_index = lax.axis_index("row")
    col_index = lax.axis_index("col")
    schur_local = schur_blocks[:, 0, :, 0]
    known_local = known_blocks[:, 0, :, 0]
    pairs_local = eigen_pairs[:, 0]
    block_rows = schur_local.shape[0]
    block_cols = schur_local.shape[1]
    blocks_total = block_rows * row_count
    band_width = FIRST + DIAGS
    row_slots = -(-band_width // col_count)
    col_slots = -(-band_width // row_count)
    per_row = -(-DIAGS // col_count)
    row_ids = jnp.arange(block_rows, dtype=jnp.int32) * row_count + row_index
    col_ids = jnp.arange(block_cols, dtype=jnp.int32) * col_count + col_index
    band_range = jnp.arange(band_width, dtype=jnp.int32)
    row_range = jnp.arange(block_rows, dtype=jnp.int32)
    row_offsets = (
        jnp.mod(col_index - row_ids, col_count)[:, None]
        + jnp.arange(row_slots, dtype=jnp.int32)[None, :] * col_count
    )
    row_reach = row_ids[:, None] + row_offsets
    row_valid = (row_offsets < band_width) & (row_reach < blocks_total)
    row_pick = jnp.clip(row_reach // col_count, 0, block_cols - 1)
    known_send = jnp.where(
        row_valid[..., None, None], pick_rows(known_local, row_pick), 0.0
    ).astype(jnp.bfloat16)
    schur_send = jnp.where(row_valid[..., None, None], pick_rows(schur_local, row_pick), 0)
    known_recv, schur_recv = (
        lax.all_gather(known_send[None], "col", axis=0, tiled=True),
        lax.all_gather(schur_send[None], "col", axis=0, tiled=True),
    )
    row_source = jnp.mod(row_ids[:, None] + band_range[None, :], col_count)
    row_slot = (band_range // col_count)[None, :]
    known_rows = known_recv[row_source, row_range[:, None], row_slot]
    schur_rows = schur_recv[row_source, row_range[:, None], row_slot]
    col_offsets = (
        jnp.mod(col_ids - row_index, row_count)[:, None]
        + jnp.arange(col_slots, dtype=jnp.int32)[None, :] * row_count
    )
    col_reach = col_ids[:, None] - col_offsets
    col_valid = (col_offsets < band_width) & (col_reach >= 0)
    col_pick = jnp.clip(col_reach // row_count, 0, block_rows - 1)
    known_down = jnp.where(
        col_valid[..., None, None], pick_rows(jnp.swapaxes(known_local, 0, 1), col_pick), 0.0
    ).astype(jnp.bfloat16)
    schur_down = jnp.where(
        col_valid[..., None, None], pick_rows(jnp.swapaxes(schur_local, 0, 1), col_pick), 0
    )
    target_first = -((col_index - row_ids - FIRST) // col_count)
    target_block = target_first[:, None] + jnp.arange(per_row, dtype=jnp.int32)[None, :]
    target_cols = target_block * col_count + col_index
    distance = target_cols - row_ids[:, None]
    active = (target_block < block_cols) & (distance <= FIRST + DIAGS - 1)
    target_clip = jnp.clip(target_block, 0, block_cols - 1)
    own_strip = jnp.stack([known_down, schur_down])
    collected = jnp.zeros((row_count,) + own_strip.shape, jnp.bfloat16)
    collected = collected.at[row_index].set(own_strip)
    reach_rows = min(row_count, band_width)
    carried = own_strip
    for step in range(1, reach_rows):
        carried = shifted(carried, "row", row_count - 1)
        collected = collected.at[jnp.mod(row_index + step, row_count)].set(carried)
    known_all = collected[:, 0]
    schur_all = collected[:, 1]
    col_source = jnp.mod(target_cols[:, :, None] - band_range[None, None, :], row_count)
    col_slot = (band_range // row_count)[None, None, :]
    known_cols = known_all[col_source, target_clip[:, :, None], col_slot]
    schur_cols = schur_all[col_source, target_clip[:, :, None], col_slot]
    offsets = jnp.broadcast_to(band_range[None, None, :], col_source.shape)
    totals = right_terms(
        known_rows,
        schur_rows,
        known_cols,
        schur_cols,
        offsets,
        jnp.ones(offsets.shape, jnp.bool_),
        distance,
    )
    kept_cols = schur_cols[:, :, :DIAGS]
    pair_list = []
    for distance_now in range(FIRST, FIRST + DIAGS):
        lag = distance_now % row_count
        receiver = jnp.mod(row_index - lag, row_count)
        wanted = jnp.clip(
            (row_range * row_count + receiver + distance_now) // row_count, 0, block_rows - 1
        )
        sending = pairs_local[wanted]
        if lag == 0:
            pair_list.append(sending)
        else:
            pair_list.append(
                shifted(sending.astype(jnp.bfloat16), "row", row_count - lag).astype(sending.dtype)
            )
    vec_left = pairs_local[:, 0]
    inv_left = pairs_local[:, 1]
    lam_left = eigenvalues[row_ids]
    output = known_local
    for distance_now in range(FIRST, FIRST + DIAGS):
        hitting = active & (distance == distance_now)
        solving = jnp.any(hitting, axis=1)
        chosen = jnp.sum(jnp.where(hitting[..., None, None], totals, 0.0), axis=1)
        block_col = jnp.sum(jnp.where(hitting, target_clip, 0), axis=1)
        block_ids = jnp.clip(block_col * col_count + col_index, 0, blocks_total - 1)
        vec_right = pair_list[distance_now - FIRST][:, 0]
        inv_right = pair_list[distance_now - FIRST][:, 1]
        lam_right = eigenvalues[block_ids]
        spacing = lam_left[:, :, None] - lam_right[:, None, :]
        spacing = jnp.where(solving[:, None, None], spacing, 1.0)
        mixed_block = full_dot(full_dot(inv_left, chosen), vec_right) / spacing
        solved = full_dot(full_dot(vec_left, mixed_block), inv_right)
        solved = jnp.where(solving[:, None, None], solved, 0.0)
        placing = solving[:, None] & (
            jnp.arange(block_cols, dtype=jnp.int32)[None, :] == block_col[:, None]
        )
        output = jnp.where(placing[:, :, None, None], solved[:, None], output)
        if distance_now < FIRST + DIAGS - 1:
            rounded = solved.astype(jnp.bfloat16)
            for gap in range(1, FIRST + DIAGS - distance_now):
                row_new = shifted(rounded, "col", gap)
                receiver = jnp.mod(row_index - gap, row_count)
                wanted = jnp.clip(
                    (row_range * row_count + receiver + gap) // row_count, 0, block_rows - 1
                )
                col_new = shifted(rounded[wanted], "row", row_count - gap)
                growing = active & (distance - distance_now == gap)
                known_from_row = row_new[:, None]
                known_from_col = col_new[:, None]
                schur_from_row = schur_rows[:, gap][:, None]
                schur_from_col = kept_cols[:, :, gap]
                left_side = jnp.stack(
                    [
                        jnp.where(growing[..., None, None], known_from_row, 0),
                        jnp.where(growing[..., None, None], -schur_from_row, 0),
                    ],
                    axis=2,
                )
                right_side = jnp.stack([schur_from_col, known_from_col], axis=2)
                totals = totals + jnp.einsum(
                    "atepq,ateqr->atpr", left_side, right_side, preferred_element_type=jnp.float32
                )
    return output[:, None, :, None]


ROUNDS = {0: [[(0, 1)], [(0, 2)]], 1: [[(1, 2), (0, 3)], [(1, 3)]], 2: [[(2, 3)]]}


def lag_of(r, c, cols):
    return lax.rem(c - r + 2 * cols * FIRST, cols)


def lead_of(r, c, cols):
    return lax.div(r - c + lag_of(r, c, cols), cols)


def any_spec():
    return pl.BlockSpec(memory_space=pltpu.HBM)


def place_spec():
    return pl.BlockSpec(memory_space=pltpu.SMEM)


def mod_add(value, shift, size):
    return lax.rem(value + shift + 4 * size, size)


def mirrored(step, c, cols):
    return jnp.where(c >= cols // 2, -step, step)


def column_picks(place, step, chips, aim_core, rows, cols, a):
    r, c = place[0], place[1]
    chip = mod_add(lax.div(r, 2), -step, chips)
    lead = lead_of(2 * chip + aim_core, c, cols)
    j = rows * a + FIRST + cols * lead + c
    off_f = lax.rem(j - r + rows, rows)
    off_s = 1 + lax.rem(j - r - 1 + rows, rows)
    return lax.div(j - off_f - r, rows), lax.div(j - off_s - r, rows), (j - c) // cols


def pack(known, schur, place, aim_core, rows, cols, first):
    block_rows, block_cols, bs = known.shape[0], known.shape[1], known.shape[2]
    count = block_rows - 1
    chips = rows // 2
    slots = FIRST // cols

    n_rows = slots if first else 0
    shapes = [(count, 2, bs, bs)] * (n_rows + chips) + ([(count, bs, bs)] if first else [])
    total = count * (n_rows + chips)

    def kernel(place, known_ref, schur_ref, *refs):
        outs, refs = refs[: len(shapes)], refs[len(shapes) :]
        bufs, refs = refs[: len(shapes)], refs[len(shapes) :]
        wide, in_sems, out_sems, far_sems = refs
        r, c = place[0], place[1]
        lead = lead_of(r, c, cols)
        groups = []
        for step in [chips // 2] + [x for x in range(1, chips) if x != chips // 2] + [0]:
            picks = []
            for a in range(count):
                way = step if first else mirrored(step, c, cols)
                f_row, s_row, b = column_picks(place, way, chips, aim_core, rows, cols, a)
                picks.append(((f_row, b), (s_row, b)))
            groups.append((n_rows + step, picks))
        extra = jnp.where(lag_of(r, c, cols) == 0, 1, 0)
        for slot in range(n_rows):
            picks = []
            for a in range(count):
                base = (rows // cols) * a + lead + slot
                picks.append(((a, base), (a, base + extra)))
            groups.insert(1 + slot, (slot, picks))

        def clip(at):
            return jnp.clip(at[0], 0, block_rows - 1), jnp.clip(at[1], 0, block_cols - 1)

        n = 0
        plans = []
        for at, picks in groups:
            mine = []
            for a, (f_at, s_at) in enumerate(picks):
                f_at, s_at = clip(f_at), clip(s_at)
                low = pltpu.make_async_copy(known_ref.at[f_at[0], f_at[1]], wide.at[n], in_sems.at[n, 0])
                thin = pltpu.make_async_copy(
                    schur_ref.at[s_at[0], s_at[1]], bufs[at].at[a, 1], in_sems.at[n, 1]
                )
                low.start()
                thin.start()
                mine.append((n, low, thin, a))
                n += 1
            plans.append((at, mine))
        fars = []
        if first:
            for a in range(count):
                at = clip((a, (rows // cols) * a + FIRST // cols + lead))
                far = pltpu.make_async_copy(schur_ref.at[at[0], at[1]], bufs[-1].at[a], far_sems.at[a])
                far.start()
                fars.append(far)
        sends = []
        for at, mine in plans:
            for n, low, thin, a in mine:
                low.wait()
                bufs[at][a, 0] = wide[n].astype(jnp.bfloat16)
                thin.wait()
            out = pltpu.make_async_copy(bufs[at], outs[at], out_sems.at[at])
            out.start()
            sends.append(out)
        if first:
            for far in fars:
                far.wait()
            out = pltpu.make_async_copy(bufs[-1], outs[-1], out_sems.at[len(shapes) - 1])
            out.start()
            sends.append(out)
        for out in sends:
            out.wait()

    return pl.pallas_call(
        kernel,
        in_specs=[place_spec(), any_spec(), any_spec()],
        out_specs=[any_spec()] * len(shapes),
        out_shape=[jax.ShapeDtypeStruct(x, jnp.bfloat16) for x in shapes],
        scratch_shapes=[pltpu.VMEM(x, jnp.bfloat16) for x in shapes]
        + [
            pltpu.VMEM((total, bs, bs), jnp.float32),
            pltpu.SemaphoreType.DMA((total, 2)),
            pltpu.SemaphoreType.DMA((len(shapes),)),
            pltpu.SemaphoreType.DMA((count,)),
        ],
        compiler_params=pltpu.CompilerParams(vmem_limit_bytes=VMEM_BYTES),
        cost_estimate=pl.CostEstimate(
            flops=total * bs * bs * 200, bytes_accessed=total * bs * bs * 10, transcendentals=0
        ),
        name="pack_first" if first else "pack_late",
    )(place, known, schur)


def copy_blocks(known):
    block_rows, block_cols, bs = known.shape[0], known.shape[1], known.shape[2]

    def kernel(source, out):
        out[...] = source[...]

    spec = pl.BlockSpec((1, block_cols, bs, bs), lambda n: (n, 0, 0, 0))
    return pl.pallas_call(
        kernel,
        grid=(block_rows,),
        in_specs=[spec],
        out_specs=spec,
        out_shape=jax.ShapeDtypeStruct(known.shape, known.dtype),
        compiler_params=pltpu.CompilerParams(vmem_limit_bytes=VMEM_BYTES),
        cost_estimate=pl.CostEstimate(
            flops=known.size * 1000, bytes_accessed=known.size * 8, transcendentals=0
        ),
        name="copy_known",
    )(known)


def mm(left, right):
    return jnp.dot(left, right, preferred_element_type=jnp.float32)


def own_lag(place, cols):
    r, c = place[0], place[1]
    lag = lag_of(r, c, cols)
    return r, c, lag, (lax.rem(r, 2) == 1) & (lag == cols - 1)


def offsets_of(r, lag, step, crossed, rows):
    chip = mod_add(lax.div(r, 2), step, rows // 2)
    core = lax.rem(r, 2)
    origin = 2 * chip + (1 - core if crossed else core)
    aim = r + lag
    return lax.rem(aim - origin + rows, rows), 1 + lax.rem(aim - origin - 1 + 2 * rows, rows)


def sum_base(place, row_parts, columns, after, own_far, row_far, col_far, late, rows, cols):
    count, _, bs, _ = row_parts[0][0].shape
    slots = len(row_parts[0])
    reach = FIRST + DIAGS - 1
    far_in = [own_far] + row_far + col_far
    flat_rows = [x for parts in row_parts for x in parts]
    n_rows, n_cols, n_far, n_after = len(flat_rows), len(columns), len(far_in), len(after)

    def kernel(place, *refs):
        row_in, refs = refs[:n_rows], refs[n_rows:]
        col_in, refs = refs[:n_cols], refs[n_cols:]
        far_ref, refs = refs[:n_far], refs[n_far:]
        outs, refs = refs[: 3 + (1 if n_after else 0)], refs[3 + (1 if n_after else 0) :]
        total_out, keep_row, keep_col = outs[:3]
        row_f, row_s, col_buf, col_far_buf, left_buf, total, sems = refs
        r, c, lag, is_late = own_lag(place, cols)
        active = is_late if late else jnp.logical_not(is_late)

        @pl.when(active)
        def _():
            sem = 0

            def plan(src, dst):
                nonlocal sem
                copy = pltpu.make_async_copy(src, dst, sems.at[sem])
                sem += 1
                return copy

            def begin(src, dst):
                copy = plan(src, dst)
                copy.start()
                return copy

            copies = []
            for n, ref in enumerate(row_in):
                shift = lag_of(r, jnp.bitwise_xor(c, n // slots), cols)
                shift_s = lax.rem(shift + cols - 1, cols)
                slot = n % slots
                copies.append(begin(ref.at[:, 0], row_f.at[:, cols * slot + shift]))
                copies.append(begin(ref.at[:, 1], row_s.at[:, cols * slot + shift_s]))
            far_rows = []
            for g in range(1 + len(row_far)):
                copy = plan(far_ref[g], row_s.at[:, jnp.maximum(FIRST + lag - g - 1, FIRST)])
                pl.when(lag > g)(copy.start)
                far_rows.append((g, copy))
            for g in range(1 + len(col_far)):
                src = far_ref[0] if g == 0 else far_ref[len(row_far) + g]
                copies.append(begin(src, col_far_buf.at[g]))
            col_copies = [begin(ref, col_buf.at[n]) for n, ref in enumerate(col_in)]
            for copy in copies:
                copy.wait()
            for g, copy in far_rows:
                pl.when(lag > g)(copy.wait)
            keeps = [(None, begin(row_s.at[:, pl.ds(0, DIAGS - 1)], keep_row))]

            def lefts(step, crossed, a):
                way = mirrored(step, c, cols) if late else step
                off_f, off_s = offsets_of(r, lag, way, crossed, rows)
                at_f = FIRST + lag - off_s
                left = row_f[a, jnp.minimum(at_f, FIRST - 1)]
                left = jnp.where(at_f < FIRST, left, jnp.zeros_like(left))
                return left, row_s[a, FIRST + lag - off_f - 1]

            for n, (step, crossed) in enumerate(after):
                for a in range(count):
                    left_buf[a, 2 * n], left_buf[a, 2 * n + 1] = lefts(step, crossed, a)
            if n_after:
                keeps.append((None, begin(left_buf, outs[3])))
            for a in range(count):
                part = jnp.zeros((bs, bs), jnp.float32)
                for g in range(1 + len(col_far)):
                    at = jnp.where(r + g >= rows, jnp.minimum(a + 1, count - 1), a)
                    left = row_f[a, g]
                    left = jnp.where(lag > g, left, jnp.zeros_like(left))
                    part = part + mm(left, col_far_buf[g, at])
                total[a] = part
            for n, (_, step, crossed) in enumerate(columns):
                way = mirrored(step, c, cols) if late else step
                off_s = offsets_of(r, lag, way, crossed, rows)[1]
                col_copies[n].wait()
                for a in range(count):
                    with_s, with_f = lefts(step, crossed, a)
                    total[a] += mm(with_s, col_buf[n, a, 1]) - mm(with_f, col_buf[n, a, 0])
                save = plan(col_buf.at[n, :, 1], keep_col.at[:, jnp.minimum(off_s, DIAGS - 1) - 1])
                pl.when(off_s < DIAGS)(save.start)
                keeps.append((off_s, save))
            out = begin(total, total_out)
            for off_s, copy in keeps:
                if off_s is None:
                    copy.wait()
                else:
                    pl.when(off_s < DIAGS)(copy.wait)
            out.wait()

    out_shape = [
        jax.ShapeDtypeStruct((count, bs, bs), jnp.float32),
        jax.ShapeDtypeStruct((count, DIAGS - 1, bs, bs), jnp.bfloat16),
        jax.ShapeDtypeStruct((count, DIAGS - 1, bs, bs), jnp.bfloat16),
    ]
    if n_after:
        out_shape.append(jax.ShapeDtypeStruct((count, 2 * n_after, bs, bs), jnp.bfloat16))
    return pl.pallas_call(
        kernel,
        in_specs=[place_spec()] + [any_spec()] * (n_rows + n_cols + n_far),
        out_specs=[any_spec()] * len(out_shape),
        out_shape=out_shape,
        scratch_shapes=[
            pltpu.VMEM((count, FIRST, bs, bs), jnp.bfloat16),
            pltpu.VMEM((count, reach, bs, bs), jnp.bfloat16),
            pltpu.VMEM((n_cols, count, 2, bs, bs), jnp.bfloat16),
            pltpu.VMEM((1 + len(col_far), count, bs, bs), jnp.bfloat16),
            pltpu.VMEM((count, max(2 * n_after, 1), bs, bs), jnp.bfloat16),
            pltpu.VMEM((count, bs, bs), jnp.float32),
            pltpu.SemaphoreType.DMA((2 * n_rows + n_far + 2 * n_cols + 4,)),
        ],
        compiler_params=pltpu.CompilerParams(vmem_limit_bytes=VMEM_BYTES),
        cost_estimate=pl.CostEstimate(
            flops=count * 18 * 2 * bs**3, bytes_accessed=count * 40 * bs * bs * 2, transcendentals=0
        ),
        name="sum_late" if late else "sum_early",
    )(place, *flat_rows, *[x for x, _, _ in columns], *far_in)


def sum_rest(place, columns, sums, late, rows, cols):
    total_in, keep_row, keep_col, lefts = sums
    count, bs = total_in.shape[0], total_in.shape[1]
    n_cols = len(columns)

    def kernel(place, *refs):
        col_in, refs = refs[:n_cols], refs[n_cols:]
        old, _, left_in, total_out, keep_out, col_buf, left_buf, total, sems = refs
        r, c, lag, is_late = own_lag(place, cols)

        @pl.when(is_late if late else jnp.logical_not(is_late))
        def _():
            copies = [pltpu.make_async_copy(old, total, sems.at[0])]
            copies.append(pltpu.make_async_copy(left_in, left_buf, sems.at[1]))
            for n, ref in enumerate(col_in):
                copies.append(pltpu.make_async_copy(ref, col_buf.at[n], sems.at[2 + n]))
            for copy in copies:
                copy.start()
            for copy in copies:
                copy.wait()
            saves = []
            for n, (_, step, crossed) in enumerate(columns):
                way = mirrored(step, c, cols) if late else step
                off_s = offsets_of(r, lag, way, crossed, rows)[1]
                save = pltpu.make_async_copy(
                    col_buf.at[n, :, 1],
                    keep_out.at[:, jnp.minimum(off_s, DIAGS - 1) - 1],
                    sems.at[2 + n],
                )
                pl.when(off_s < DIAGS)(save.start)
                saves.append((off_s, save))
            for a in range(count):
                part = total[a]
                for n in range(n_cols):
                    part = part + mm(left_buf[a, 2 * n], col_buf[n, a, 1])
                    part = part - mm(left_buf[a, 2 * n + 1], col_buf[n, a, 0])
                total[a] = part
            out = pltpu.make_async_copy(total, total_out, sems.at[0])
            out.start()
            for off_s, save in saves:
                pl.when(off_s < DIAGS)(save.wait)
            out.wait()

    first = 1 + n_cols
    total, keep_col = pl.pallas_call(
        kernel,
        in_specs=[place_spec()] + [any_spec()] * (n_cols + 3),
        out_specs=[any_spec()] * 2,
        out_shape=[
            jax.ShapeDtypeStruct(total_in.shape, total_in.dtype),
            jax.ShapeDtypeStruct(keep_col.shape, keep_col.dtype),
        ],
        input_output_aliases={first: 0, first + 1: 1},
        scratch_shapes=[
            pltpu.VMEM((n_cols, count, 2, bs, bs), jnp.bfloat16),
            pltpu.VMEM(lefts.shape, jnp.bfloat16),
            pltpu.VMEM((count, bs, bs), jnp.float32),
            pltpu.SemaphoreType.DMA((2 + n_cols,)),
        ],
        compiler_params=pltpu.CompilerParams(vmem_limit_bytes=VMEM_BYTES),
        cost_estimate=pl.CostEstimate(
            flops=count * 4 * 2 * bs**3, bytes_accessed=count * 12 * bs * bs * 2, transcendentals=0
        ),
        name="rest_late" if late else "sum_rest",
    )(place, *[x for x, _, _ in columns], total_in, keep_col, lefts)
    return total, keep_row, keep_col


def halves(value):
    high = value.astype(jnp.bfloat16)
    return high, (value - high.astype(jnp.float32)).astype(jnp.bfloat16)


def solve_stage(
    stage, place, output, carried, sums, late_sums, row_new, col_new, far_pairs, own_pairs, spacing, rows, cols
):
    count, bs = sums[0].shape[0], sums[0].shape[1]
    block_cols = output.shape[1]
    last = stage == DIAGS - 1
    two = last and late_sums is not None
    groups = [list(sums)] + ([list(late_sums)] if two else [])
    flat = [x for group in groups for x in group]
    n_new = len(row_new)

    passed = [] if carried is None else [carried]

    def kernel(place, out_in, *refs):
        refs = refs[len(passed) :]
        sum_groups, refs = refs[: len(flat)], refs[len(flat) :]
        row_in, refs = refs[:n_new], refs[n_new:]
        col_in, refs = refs[:n_new], refs[n_new:]
        pair_far, pair_own, space_in, out, sent, refs = *refs[:5], refs[5:]
        total, keep_r, keep_c, row_buf, col_buf, far_buf, own_buf, space, solved, narrow, sems = refs
        r, c = place[0], place[1]
        lag = lag_of(r, c, cols)
        is_late = (lax.rem(r, 2) == 1) & (lag == cols - 1)

        @pl.when(lag == stage)
        def _():
            sem = 0

            def plan(src, dst):
                nonlocal sem
                copy = pltpu.make_async_copy(src, dst, sems.at[sem])
                sem += 1
                return copy

            news = []
            for n in range(n_new):
                news.append(plan(row_in[n], row_buf.at[n]))
                news.append(plan(col_in[n], col_buf.at[n]))
            rest = [
                plan(pair_own.at[pl.ds(0, count)], own_buf),
                plan(pair_far, far_buf),
                plan(space_in, space),
            ]
            near = pl.ds(0, max(stage, 1))
            targets = [(0, total)]
            if n_new:
                targets += [(1, keep_r.at[:, near]), (2, keep_c.at[:, near])]
            first_sem = sem

            def load(group, i, dst):
                src = group[i].at[:, near] if i else group[i]
                return pltpu.make_async_copy(src, dst, sems.at[first_sem + i])

            for at, group in enumerate([sum_groups[:3], sum_groups[3:]][: len(groups)]):
                chosen = is_late if at == 1 else jnp.logical_not(is_late)
                for i, dst in targets:
                    if two:
                        pl.when(chosen)(load(group, i, dst).start)
                    else:
                        load(group, i, dst).start()
            for copy in news + rest:
                copy.start()
            for i, dst in targets:
                load(sum_groups, i, dst).wait()
            for copy in news:
                copy.wait()
            lead = lead_of(r, c, cols)
            wrapped = jnp.where(r + lag >= rows, 1, 0)
            each = range(count)
            right = [total[a] for a in each]
            for n in range(n_new):
                g = stage - n
                for a in each:
                    at = jnp.where(r + g >= rows, jnp.minimum(a + 1, count - 1), a)
                    right[a] = right[a] + mm(row_buf[n, a], keep_c[a, g - 1])
                    right[a] = right[a] - mm(keep_r[a, g - 1], col_buf[n, at])
            far = [jnp.minimum(a + wrapped, count - 1) for a in each]
            for copy in rest:
                copy.wait()

            def from_left(side, values):
                left = [halves(own_buf[a, side]) for a in each]
                value = [halves(x) for x in values]
                return [
                    mm(left[a][0], value[a][0])
                    + (mm(left[a][0], value[a][1]) + mm(left[a][1], value[a][0]))
                    for a in each
                ]

            def from_right(values, side):
                value = [halves(x) for x in values]
                return [
                    mm(value[a][0], far_buf[far[a], side]) + mm(value[a][1], far_buf[far[a], side])
                    for a in each
                ]

            mixed = from_right(from_left(1, right), 0)
            mixed = [mixed[a] / space[a] for a in each]
            answer = from_right(from_left(0, mixed), 1)
            for a in each:
                narrow[a] = answer[a].astype(jnp.bfloat16)
                solved[a] = answer[a]
            copies = []
            send = None
            if not last:
                send = pltpu.make_async_copy(narrow, sent, sems.at[sem])
                send.start()
            for a in range(count):
                at = (rows // cols) * a + FIRST // cols + lead
                copy = pltpu.make_async_copy(
                    solved.at[a], out.at[a, jnp.minimum(at, block_cols - 1)], sems.at[a]
                )
                pl.when(at < block_cols)(copy.start)
                copies.append((at, copy))
            for at, copy in copies:
                pl.when(at < block_cols)(copy.wait)
            if send is not None:
                send.wait()

    n_in = 2 + len(passed) + len(flat) + 2 * n_new + 3
    half = max(n_new, 1)
    return pl.pallas_call(
        kernel,
        in_specs=[place_spec()] + [any_spec()] * (n_in - 1),
        out_specs=[any_spec()] * 2,
        out_shape=[
            jax.ShapeDtypeStruct(output.shape, output.dtype),
            jax.ShapeDtypeStruct((count, bs, bs), jnp.bfloat16),
        ],
        input_output_aliases={1 + i: i for i in range(1 + len(passed))},
        scratch_shapes=[
            pltpu.VMEM((count, bs, bs), jnp.float32),
            pltpu.VMEM((count, DIAGS - 1, bs, bs), jnp.bfloat16),
            pltpu.VMEM((count, DIAGS - 1, bs, bs), jnp.bfloat16),
            pltpu.VMEM((half, count, bs, bs), jnp.bfloat16),
            pltpu.VMEM((half, count, bs, bs), jnp.bfloat16),
            pltpu.VMEM((count, 2, bs, bs), jnp.bfloat16),
            pltpu.VMEM((count, 2, bs, bs), jnp.float32),
            pltpu.VMEM((count, bs, bs), jnp.float32),
            pltpu.VMEM((count, bs, bs), jnp.float32),
            pltpu.VMEM((count, bs, bs), jnp.bfloat16),
            pltpu.SemaphoreType.DMA((2 * n_new + 6 + count,)),
        ],
        compiler_params=pltpu.CompilerParams(vmem_limit_bytes=VMEM_BYTES),
        cost_estimate=pl.CostEstimate(
            flops=count * 12 * 2 * bs**3, bytes_accessed=count * 20 * bs * bs * 2, transcendentals=0
        ),
    )(place, output, *passed, *flat, *row_new, *col_new, far_pairs, own_pairs, spacing)


def banded_body(schur_blocks, known_blocks, eigen_pairs, eigenvalues):
    return banded_steps(schur_blocks, known_blocks, eigen_pairs, eigenvalues)


def banded_steps(schur_blocks, known_blocks, eigen_pairs, eigenvalues):
    rows = lax.axis_size("row")
    cols = lax.axis_size("col")
    r = lax.axis_index("row")
    c = lax.axis_index("col")
    schur = schur_blocks[:, 0, :, 0]
    known = known_blocks[:, 0, :, 0]
    pairs = eigen_pairs[:, 0]
    count = known.shape[0] - 1
    chips = rows // 2
    slots = FIRST // cols
    devices = [(i, k) for i in range(rows) for k in range(cols)]

    def lag(i, k):
        return (k - i) % cols

    def send(block, move, keep=lambda i, k: True, senders=None):
        routes = []
        for i, k in devices:
            if senders is not None and lag(i, k) not in senders:
                continue
            to = move(i, k)
            to = (to[0] % rows, to[1] % cols)
            if keep(*to):
                routes.append((i * cols + k, to[0] * cols + to[1]))
        return lax.ppermute(block, ("row", "col"), routes)

    def late_core(i, k):
        return lag(i, k) == cols - 1 and i % 2 == 1

    place = jnp.stack([r, c]).astype(jnp.int32)
    packed = pack(known, schur, place, 0, rows, cols, True)
    own_parts, col_packs, own_far = packed[:slots], packed[slots:-1], packed[-1]
    early = {0: col_packs[0]}
    for step in range(1, chips):
        early[step] = send(col_packs[step], lambda i, j, s=step: (i - 2 * s, j))
    row_parts = [list(own_parts)]
    for k in (1, 2):
        row_parts.append([send(part, lambda i, j, k=k: (i, j ^ k)) for part in own_parts])
    row_parts.append(
        [
            send(row_parts[1][0], lambda i, j: (i, j ^ 2)),
            send(row_parts[2][1], lambda i, j: (i, j ^ 1)),
        ]
    )
    row_far, col_far = [], []
    for g in range(1, DIAGS - 1):
        takes = lambda i, k, g=g: lag(i, k) > g
        row_far.append(send(own_far, lambda i, j, g=g: (i, j + g), takes))
        col_far.append(send(own_far, lambda i, j, g=g: (i - g, j), takes))
    pair_list = [lax.optimization_barrier((pairs, own_far))[0][1:].astype(jnp.bfloat16)]
    for g in range(1, DIAGS):
        takes = lambda i, k, g=g: lag(i, k) == g
        pair_list.append(send(pair_list[-1], lambda i, j: (i - 1, j), takes))
    lag_here = lag_of(r, c, cols)
    own_ids = jnp.arange(count, dtype=jnp.int32) * rows + r
    far_ids = jnp.minimum(own_ids + FIRST + lag_here, eigenvalues.shape[0] - 1)
    spacing = eigenvalues[own_ids][:, :, None] - eigenvalues[far_ids][:, None, :]
    known_later, spacing = lax.optimization_barrier((known, spacing))
    late_packs = pack(known, schur, place, 1, rows, cols, False)
    output = copy_blocks(known_later)

    crossed = {n: send(early[n], lambda i, j: (i ^ 1, j)) for n in range(chips)}
    late = [(late_packs[0], 0, False)]
    late_last = []
    for step in range(chips):

        def onward(i, j, step=step):
            return i - 2 * (step if j < cols // 2 else -step), j

        def onward_across(i, j, onward=onward):
            return onward(i, j)[0] ^ 1, j

        into = late_last if step else late
        if step:
            into.append((send(late_packs[step], onward, late_core), step, False))
        into.append((send(late_packs[step], onward_across, late_core), step, True))
    final = chips // 2
    last = [(early[final], final, False), (crossed[final], final, True)]
    ready = []
    for step in range(chips):
        if step != final:
            ready += [(early[step], step, False), (crossed[step], step, True)]
    sums = sum_base(
        place, row_parts, ready, [x[1:] for x in last], own_far, row_far, col_far, False, rows, cols
    )
    sums = sum_rest(place, last, sums, False, rows, cols)
    late_sums = sum_base(
        place, row_parts, late, [x[1:] for x in late_last], own_far, row_far, col_far, True, rows, cols
    )
    late_sums = sum_rest(place, late_last, late_sums, True, rows, cols)
    carried = None
    row_new = {}
    col_new = {}
    for stage in range(DIAGS):
        output, carried = solve_stage(
            stage,
            place,
            output,
            carried,
            sums,
            late_sums,
            [row_new[n, stage] for n in range(stage)],
            [col_new[n, stage] for n in range(stage)],
            pair_list[stage],
            pairs,
            spacing,
            rows,
            cols,
        )
        for hops in ROUNDS.get(stage, ()):
            by_lag = dict(hops)
            takes = set(by_lag.values())

            def gap(i, k):
                return by_lag.get(lag(i, k), lag(i, k)) - lag(i, k)

            def wanted(i, k):
                return lag(i, k) in takes

            across = send(carried, lambda i, j: (i, j + gap(i, j)), wanted, by_lag)
            upward = send(carried, lambda i, j: (i - gap(i, j), j), wanted, by_lag)
            for hop in hops:
                row_new[hop] = across
                col_new[hop] = upward
    return output[:, None, :, None]


def solution(mesh):
    rows, cols = mesh.shape["row"], mesh.shape["col"]
    banded = rows == FIRST and cols == DIAGS
    return jax.shard_map(
        banded_body if banded else body,
        mesh=mesh,
        in_specs=(
            P(None, "row", None, "col", None, None),
            P(None, "row", None, "col", None, None),
            P(None, "row", None, None, None),
            P(),
        ),
        out_specs=P(None, "row", None, "col", None, None),
        check_vma=False,
    )
```

```python
import jax
import jax.numpy as jnp
from jax import lax
from jax.experimental import pallas as pl
from jax.experimental.pallas import tpu as pltpu
from jax.sharding import PartitionSpec as P


FIRST = 8
DIAGS = 4
VMEM_BYTES = 67_043_328


def shifted(block, axis, distance):
    devices = range(lax.axis_size(axis))
    route = [((i - distance) % len(devices), i) for i in devices]
    return lax.ppermute(block, axis, route)


def pick_rows(stacked, indices):
    return jax.vmap(lambda source, chosen: source[chosen])(stacked, indices)


def full_dot(left_side, right_side):
    return jnp.einsum(
        "apq,aqr->apr",
        left_side,
        right_side,
        precision=lax.Precision.HIGHEST,
        preferred_element_type=jnp.float32,
    )


def right_terms(known_rows, schur_rows, known_cols, schur_cols, offsets, usable, distance):
    band_width = known_rows.shape[1]
    reach_back = distance[:, :, None] - offsets
    first_mask = usable & (offsets >= 1) & (reach_back >= 0) & (reach_back <= FIRST - 1)
    second_mask = usable & (offsets <= FIRST - 1) & (reach_back >= 1)
    clipped = jnp.clip(reach_back, 0, band_width - 1)
    known_pick = jnp.where(first_mask[..., None, None], pick_rows(known_rows, clipped), 0)
    schur_pick = jnp.where(second_mask[..., None, None], -pick_rows(schur_rows, clipped), 0)
    left_side = jnp.concatenate([known_pick, schur_pick], axis=2)
    right_side = jnp.concatenate([schur_cols, known_cols], axis=2)
    return jnp.einsum(
        "atepq,ateqr->atpr", left_side, right_side, preferred_element_type=jnp.float32
    )


def body(schur_blocks, known_blocks, eigen_pairs, eigenvalues):
    row_count = lax.axis_size("row")
    col_count = lax.axis_size("col")
    row_index = lax.axis_index("row")
    col_index = lax.axis_index("col")
    schur_local = schur_blocks[:, 0, :, 0]
    known_local = known_blocks[:, 0, :, 0]
    pairs_local = eigen_pairs[:, 0]
    block_rows = schur_local.shape[0]
    block_cols = schur_local.shape[1]
    blocks_total = block_rows * row_count
    band_width = FIRST + DIAGS
    row_slots = -(-band_width // col_count)
    col_slots = -(-band_width // row_count)
    per_row = -(-DIAGS // col_count)
    row_ids = jnp.arange(block_rows, dtype=jnp.int32) * row_count + row_index
    col_ids = jnp.arange(block_cols, dtype=jnp.int32) * col_count + col_index
    band_range = jnp.arange(band_width, dtype=jnp.int32)
    row_range = jnp.arange(block_rows, dtype=jnp.int32)
    row_offsets = (
        jnp.mod(col_index - row_ids, col_count)[:, None]
        + jnp.arange(row_slots, dtype=jnp.int32)[None, :] * col_count
    )
    row_reach = row_ids[:, None] + row_offsets
    row_valid = (row_offsets < band_width) & (row_reach < blocks_total)
    row_pick = jnp.clip(row_reach // col_count, 0, block_cols - 1)
    known_send = jnp.where(
        row_valid[..., None, None], pick_rows(known_local, row_pick), 0.0
    ).astype(jnp.bfloat16)
    schur_send = jnp.where(row_valid[..., None, None], pick_rows(schur_local, row_pick), 0)
    known_recv, schur_recv = (
        lax.all_gather(known_send[None], "col", axis=0, tiled=True),
        lax.all_gather(schur_send[None], "col", axis=0, tiled=True),
    )
    row_source = jnp.mod(row_ids[:, None] + band_range[None, :], col_count)
    row_slot = (band_range // col_count)[None, :]
    known_rows = known_recv[row_source, row_range[:, None], row_slot]
    schur_rows = schur_recv[row_source, row_range[:, None], row_slot]
    col_offsets = (
        jnp.mod(col_ids - row_index, row_count)[:, None]
        + jnp.arange(col_slots, dtype=jnp.int32)[None, :] * row_count
    )
    col_reach = col_ids[:, None] - col_offsets
    col_valid = (col_offsets < band_width) & (col_reach >= 0)
    col_pick = jnp.clip(col_reach // row_count, 0, block_rows - 1)
    known_down = jnp.where(
        col_valid[..., None, None], pick_rows(jnp.swapaxes(known_local, 0, 1), col_pick), 0.0
    ).astype(jnp.bfloat16)
    schur_down = jnp.where(
        col_valid[..., None, None], pick_rows(jnp.swapaxes(schur_local, 0, 1), col_pick), 0
    )
    target_first = -((col_index - row_ids - FIRST) // col_count)
    target_block = target_first[:, None] + jnp.arange(per_row, dtype=jnp.int32)[None, :]
    target_cols = target_block * col_count + col_index
    distance = target_cols - row_ids[:, None]
    active = (target_block < block_cols) & (distance <= FIRST + DIAGS - 1)
    target_clip = jnp.clip(target_block, 0, block_cols - 1)
    own_strip = jnp.stack([known_down, schur_down])
    collected = jnp.zeros((row_count,) + own_strip.shape, jnp.bfloat16)
    collected = collected.at[row_index].set(own_strip)
    reach_rows = min(row_count, band_width)
    carried = own_strip
    for step in range(1, reach_rows):
        carried = shifted(carried, "row", row_count - 1)
        collected = collected.at[jnp.mod(row_index + step, row_count)].set(carried)
    known_all = collected[:, 0]
    schur_all = collected[:, 1]
    col_source = jnp.mod(target_cols[:, :, None] - band_range[None, None, :], row_count)
    col_slot = (band_range // row_count)[None, None, :]
    known_cols = known_all[col_source, target_clip[:, :, None], col_slot]
    schur_cols = schur_all[col_source, target_clip[:, :, None], col_slot]
    offsets = jnp.broadcast_to(band_range[None, None, :], col_source.shape)
    totals = right_terms(
        known_rows,
        schur_rows,
        known_cols,
        schur_cols,
        offsets,
        jnp.ones(offsets.shape, jnp.bool_),
        distance,
    )
    kept_cols = schur_cols[:, :, :DIAGS]
    pair_list = []
    for distance_now in range(FIRST, FIRST + DIAGS):
        lag = distance_now % row_count
        receiver = jnp.mod(row_index - lag, row_count)
        wanted = jnp.clip(
            (row_range * row_count + receiver + distance_now) // row_count, 0, block_rows - 1
        )
        sending = pairs_local[wanted]
        if lag == 0:
            pair_list.append(sending)
        else:
            pair_list.append(
                shifted(sending.astype(jnp.bfloat16), "row", row_count - lag).astype(sending.dtype)
            )
    vec_left = pairs_local[:, 0]
    inv_left = pairs_local[:, 1]
    lam_left = eigenvalues[row_ids]
    output = known_local
    for distance_now in range(FIRST, FIRST + DIAGS):
        hitting = active & (distance == distance_now)
        solving = jnp.any(hitting, axis=1)
        chosen = jnp.sum(jnp.where(hitting[..., None, None], totals, 0.0), axis=1)
        block_col = jnp.sum(jnp.where(hitting, target_clip, 0), axis=1)
        block_ids = jnp.clip(block_col * col_count + col_index, 0, blocks_total - 1)
        vec_right = pair_list[distance_now - FIRST][:, 0]
        inv_right = pair_list[distance_now - FIRST][:, 1]
        lam_right = eigenvalues[block_ids]
        spacing = lam_left[:, :, None] - lam_right[:, None, :]
        spacing = jnp.where(solving[:, None, None], spacing, 1.0)
        mixed_block = full_dot(full_dot(inv_left, chosen), vec_right) / spacing
        solved = full_dot(full_dot(vec_left, mixed_block), inv_right)
        solved = jnp.where(solving[:, None, None], solved, 0.0)
        placing = solving[:, None] & (
            jnp.arange(block_cols, dtype=jnp.int32)[None, :] == block_col[:, None]
        )
        output = jnp.where(placing[:, :, None, None], solved[:, None], output)
        if distance_now < FIRST + DIAGS - 1:
            rounded = solved.astype(jnp.bfloat16)
            for gap in range(1, FIRST + DIAGS - distance_now):
                row_new = shifted(rounded, "col", gap)
                receiver = jnp.mod(row_index - gap, row_count)
                wanted = jnp.clip(
                    (row_range * row_count + receiver + gap) // row_count, 0, block_rows - 1
                )
                col_new = shifted(rounded[wanted], "row", row_count - gap)
                growing = active & (distance - distance_now == gap)
                known_from_row = row_new[:, None]
                known_from_col = col_new[:, None]
                schur_from_row = schur_rows[:, gap][:, None]
                schur_from_col = kept_cols[:, :, gap]
                left_side = jnp.stack(
                    [
                        jnp.where(growing[..., None, None], known_from_row, 0),
                        jnp.where(growing[..., None, None], -schur_from_row, 0),
                    ],
                    axis=2,
                )
                right_side = jnp.stack([schur_from_col, known_from_col], axis=2)
                totals = totals + jnp.einsum(
                    "atepq,ateqr->atpr", left_side, right_side, preferred_element_type=jnp.float32
                )
    return output[:, None, :, None]


ROUNDS = {0: [[(0, 1)], [(0, 2)]], 1: [[(1, 2), (0, 3)], [(1, 3)]], 2: [[(2, 3)]]}


def lag_of(r, c, cols):
    return lax.rem(c - r + 2 * cols * FIRST, cols)


def lead_of(r, c, cols):
    return lax.div(r - c + lag_of(r, c, cols), cols)


def any_spec():
    return pl.BlockSpec(memory_space=pltpu.HBM)


def place_spec():
    return pl.BlockSpec(memory_space=pltpu.SMEM)


def mod_add(value, shift, size):
    return lax.rem(value + shift + 4 * size, size)


def mirrored(step, c, cols):
    return jnp.where(c >= cols // 2, -step, step)


def column_picks(place, step, chips, aim_core, rows, cols, a):
    r, c = place[0], place[1]
    chip = mod_add(lax.div(r, 2), -step, chips)
    lead = lead_of(2 * chip + aim_core, c, cols)
    j = rows * a + FIRST + cols * lead + c
    off_f = lax.rem(j - r + rows, rows)
    off_s = 1 + lax.rem(j - r - 1 + rows, rows)
    return lax.div(j - off_f - r, rows), lax.div(j - off_s - r, rows), (j - c) // cols


def pack(known, schur, place, aim_core, rows, cols, kind):
    block_rows, block_cols, bs = known.shape[0], known.shape[1], known.shape[2]
    count = block_rows - 1
    chips = rows // 2
    slots = FIRST // cols

    first = kind == "rows"
    n_rows = slots if first else 0
    n_cols = 0 if first else chips
    shapes = [(count, 2, bs, bs)] * (n_rows + n_cols) + ([(count, bs, bs)] if first else [])
    total = count * (n_rows + n_cols)
    steps = [] if first else [x for x in range(1, chips) if x != chips // 2] + [chips // 2, 0]

    def kernel(place, known_ref, schur_ref, *refs):
        outs, refs = refs[: len(shapes)], refs[len(shapes) :]
        bufs, refs = refs[: len(shapes)], refs[len(shapes) :]
        wide, in_sems, out_sems, far_sems = refs
        r, c = place[0], place[1]
        lead = lead_of(r, c, cols)
        groups = []
        for step in steps:
            picks = []
            for a in range(count):
                way = mirrored(step, c, cols) if kind == "late" else step
                f_row, s_row, b = column_picks(place, way, chips, aim_core, rows, cols, a)
                picks.append(((f_row, b), (s_row, b)))
            groups.append((n_rows + step, picks))
        extra = jnp.where(lag_of(r, c, cols) == 0, 1, 0)
        for slot in range(n_rows):
            picks = []
            for a in range(count):
                base = (rows // cols) * a + lead + slot
                picks.append(((a, base), (a, base + extra)))
            groups.append((slot, picks))

        def clip(at):
            return jnp.clip(at[0], 0, block_rows - 1), jnp.clip(at[1], 0, block_cols - 1)

        n = 0
        plans = []
        for at, picks in groups:
            mine = []
            for a, (f_at, s_at) in enumerate(picks):
                f_at, s_at = clip(f_at), clip(s_at)
                low = pltpu.make_async_copy(known_ref.at[f_at[0], f_at[1]], wide.at[n], in_sems.at[n, 0])
                thin = pltpu.make_async_copy(
                    schur_ref.at[s_at[0], s_at[1]], bufs[at].at[a, 1], in_sems.at[n, 1]
                )
                low.start()
                thin.start()
                mine.append((n, low, thin, a))
                n += 1
            plans.append((at, mine))
        fars = []
        if first:
            for a in range(count):
                at = clip((a, (rows // cols) * a + FIRST // cols + lead))
                far = pltpu.make_async_copy(schur_ref.at[at[0], at[1]], bufs[-1].at[a], far_sems.at[a])
                far.start()
                fars.append(far)
        sends = []
        for at, mine in plans:
            for n, low, thin, a in mine:
                low.wait()
                bufs[at][a, 0] = wide[n].astype(jnp.bfloat16)
                thin.wait()
            out = pltpu.make_async_copy(bufs[at], outs[at], out_sems.at[at])
            out.start()
            sends.append(out)
        if first:
            for far in fars:
                far.wait()
            out = pltpu.make_async_copy(bufs[-1], outs[-1], out_sems.at[len(shapes) - 1])
            out.start()
            sends.append(out)
        for out in sends:
            out.wait()

    return pl.pallas_call(
        kernel,
        in_specs=[place_spec(), any_spec(), any_spec()],
        out_specs=[any_spec()] * len(shapes),
        out_shape=[jax.ShapeDtypeStruct(x, jnp.bfloat16) for x in shapes],
        scratch_shapes=[pltpu.VMEM(x, jnp.bfloat16) for x in shapes]
        + [
            pltpu.VMEM((total, bs, bs), jnp.float32),
            pltpu.SemaphoreType.DMA((total, 2)),
            pltpu.SemaphoreType.DMA((len(shapes),)),
            pltpu.SemaphoreType.DMA((count,)),
        ],
        compiler_params=pltpu.CompilerParams(vmem_limit_bytes=VMEM_BYTES),
        cost_estimate=pl.CostEstimate(
            flops=total * bs * bs * 200, bytes_accessed=total * bs * bs * 10, transcendentals=0
        ),
    )(place, known, schur)


def copy_blocks(known):
    block_rows, block_cols, bs = known.shape[0], known.shape[1], known.shape[2]

    def kernel(source, out):
        out[...] = source[...]

    spec = pl.BlockSpec((1, block_cols, bs, bs), lambda n: (n, 0, 0, 0))
    return pl.pallas_call(
        kernel,
        grid=(block_rows,),
        in_specs=[spec],
        out_specs=spec,
        out_shape=jax.ShapeDtypeStruct(known.shape, known.dtype),
        compiler_params=pltpu.CompilerParams(vmem_limit_bytes=VMEM_BYTES),
        cost_estimate=pl.CostEstimate(
            flops=known.size * 1000, bytes_accessed=known.size * 8, transcendentals=0
        ),
        name="copy_known",
    )(known)


def mm(left, right):
    return jnp.dot(left, right, preferred_element_type=jnp.float32)


def own_lag(place, cols):
    r, c = place[0], place[1]
    lag = lag_of(r, c, cols)
    return r, c, lag, (lax.rem(r, 2) == 1) & (lag == cols - 1)


def offsets_of(r, lag, step, crossed, rows):
    chip = mod_add(lax.div(r, 2), step, rows // 2)
    core = lax.rem(r, 2)
    origin = 2 * chip + (1 - core if crossed else core)
    aim = r + lag
    return lax.rem(aim - origin + rows, rows), 1 + lax.rem(aim - origin - 1 + 2 * rows, rows)


def sum_base(place, row_parts, columns, after, own_far, row_far, col_far, late, rows, cols):
    count, _, bs, _ = row_parts[0][0].shape
    slots = len(row_parts[0])
    reach = FIRST + DIAGS - 1
    far_in = [own_far] + row_far + col_far
    flat_rows = [x for parts in row_parts for x in parts]
    n_rows, n_cols, n_far, n_after = len(flat_rows), len(columns), len(far_in), len(after)

    def kernel(place, *refs):
        row_in, refs = refs[:n_rows], refs[n_rows:]
        col_in, refs = refs[:n_cols], refs[n_cols:]
        far_ref, refs = refs[:n_far], refs[n_far:]
        outs, refs = refs[: 3 + (1 if n_after else 0)], refs[3 + (1 if n_after else 0) :]
        total_out, keep_row, keep_col = outs[:3]
        row_f, row_s, col_buf, col_far_buf, left_buf, total, sems = refs
        r, c, lag, is_late = own_lag(place, cols)
        active = is_late if late else jnp.logical_not(is_late)

        @pl.when(active)
        def _():
            sem = 0

            def plan(src, dst):
                nonlocal sem
                copy = pltpu.make_async_copy(src, dst, sems.at[sem])
                sem += 1
                return copy

            def begin(src, dst):
                copy = plan(src, dst)
                copy.start()
                return copy

            copies = []
            for n, ref in enumerate(row_in):
                shift = lag_of(r, jnp.bitwise_xor(c, n // slots), cols)
                shift_s = lax.rem(shift + cols - 1, cols)
                slot = n % slots
                copies.append(begin(ref.at[:, 0], row_f.at[:, cols * slot + shift]))
                copies.append(begin(ref.at[:, 1], row_s.at[:, cols * slot + shift_s]))
            far_rows = []
            for g in range(1 + len(row_far)):
                copy = plan(far_ref[g], row_s.at[:, jnp.maximum(FIRST + lag - g - 1, FIRST)])
                pl.when(lag > g)(copy.start)
                far_rows.append((g, copy))
            for g in range(1 + len(col_far)):
                src = far_ref[0] if g == 0 else far_ref[len(row_far) + g]
                copies.append(begin(src, col_far_buf.at[g]))
            col_copies = [begin(ref, col_buf.at[n]) for n, ref in enumerate(col_in)]
            for copy in copies:
                copy.wait()
            for g, copy in far_rows:
                pl.when(lag > g)(copy.wait)
            keeps = [(None, begin(row_s.at[:, pl.ds(0, DIAGS - 1)], keep_row))]

            def lefts(step, crossed, a):
                way = mirrored(step, c, cols) if late else step
                off_f, off_s = offsets_of(r, lag, way, crossed, rows)
                at_f = FIRST + lag - off_s
                left = row_f[a, jnp.minimum(at_f, FIRST - 1)]
                left = jnp.where(at_f < FIRST, left, jnp.zeros_like(left))
                return left, row_s[a, FIRST + lag - off_f - 1]

            for n, (step, crossed) in enumerate(after):
                for a in range(count):
                    left_buf[a, 2 * n], left_buf[a, 2 * n + 1] = lefts(step, crossed, a)
            if n_after:
                keeps.append((None, begin(left_buf, outs[3])))
            for a in range(count):
                part = jnp.zeros((bs, bs), jnp.float32)
                for g in range(1 + len(col_far)):
                    at = jnp.where(r + g >= rows, jnp.minimum(a + 1, count - 1), a)
                    left = row_f[a, g]
                    left = jnp.where(lag > g, left, jnp.zeros_like(left))
                    part = part + mm(left, col_far_buf[g, at])
                total[a] = part
            for n, (_, step, crossed) in enumerate(columns):
                way = mirrored(step, c, cols) if late else step
                off_s = offsets_of(r, lag, way, crossed, rows)[1]
                col_copies[n].wait()
                for a in range(count):
                    with_s, with_f = lefts(step, crossed, a)
                    total[a] += mm(with_s, col_buf[n, a, 1]) - mm(with_f, col_buf[n, a, 0])
                save = plan(col_buf.at[n, :, 1], keep_col.at[:, jnp.minimum(off_s, DIAGS - 1) - 1])
                pl.when(off_s < DIAGS)(save.start)
                keeps.append((off_s, save))
            out = begin(total, total_out)
            for off_s, copy in keeps:
                if off_s is None:
                    copy.wait()
                else:
                    pl.when(off_s < DIAGS)(copy.wait)
            out.wait()

    out_shape = [
        jax.ShapeDtypeStruct((count, bs, bs), jnp.float32),
        jax.ShapeDtypeStruct((count, DIAGS - 1, bs, bs), jnp.bfloat16),
        jax.ShapeDtypeStruct((count, DIAGS - 1, bs, bs), jnp.bfloat16),
    ]
    if n_after:
        out_shape.append(jax.ShapeDtypeStruct((count, 2 * n_after, bs, bs), jnp.bfloat16))
    return pl.pallas_call(
        kernel,
        in_specs=[place_spec()] + [any_spec()] * (n_rows + n_cols + n_far),
        out_specs=[any_spec()] * len(out_shape),
        out_shape=out_shape,
        scratch_shapes=[
            pltpu.VMEM((count, FIRST, bs, bs), jnp.bfloat16),
            pltpu.VMEM((count, reach, bs, bs), jnp.bfloat16),
            pltpu.VMEM((n_cols, count, 2, bs, bs), jnp.bfloat16),
            pltpu.VMEM((1 + len(col_far), count, bs, bs), jnp.bfloat16),
            pltpu.VMEM((count, max(2 * n_after, 1), bs, bs), jnp.bfloat16),
            pltpu.VMEM((count, bs, bs), jnp.float32),
            pltpu.SemaphoreType.DMA((2 * n_rows + n_far + 2 * n_cols + 4,)),
        ],
        compiler_params=pltpu.CompilerParams(vmem_limit_bytes=VMEM_BYTES),
        cost_estimate=pl.CostEstimate(
            flops=count * 18 * 2 * bs**3, bytes_accessed=count * 40 * bs * bs * 2, transcendentals=0
        ),
        name="sum_late" if late else "sum_early",
    )(place, *flat_rows, *[x for x, _, _ in columns], *far_in)


def sum_rest(place, columns, sums, late, rows, cols):
    total_in, keep_row, keep_col, lefts = sums
    count, bs = total_in.shape[0], total_in.shape[1]
    n_cols = len(columns)

    def kernel(place, *refs):
        col_in, refs = refs[:n_cols], refs[n_cols:]
        old, _, left_in, total_out, keep_out, col_buf, left_buf, total, sems = refs
        r, c, lag, is_late = own_lag(place, cols)

        @pl.when(is_late if late else jnp.logical_not(is_late))
        def _():
            copies = [pltpu.make_async_copy(old, total, sems.at[0])]
            copies.append(pltpu.make_async_copy(left_in, left_buf, sems.at[1]))
            for n, ref in enumerate(col_in):
                copies.append(pltpu.make_async_copy(ref, col_buf.at[n], sems.at[2 + n]))
            for copy in copies:
                copy.start()
            for copy in copies:
                copy.wait()
            saves = []
            for n, (_, step, crossed) in enumerate(columns):
                way = mirrored(step, c, cols) if late else step
                off_s = offsets_of(r, lag, way, crossed, rows)[1]
                save = pltpu.make_async_copy(
                    col_buf.at[n, :, 1],
                    keep_out.at[:, jnp.minimum(off_s, DIAGS - 1) - 1],
                    sems.at[2 + n],
                )
                pl.when(off_s < DIAGS)(save.start)
                saves.append((off_s, save))
            for a in range(count):
                part = total[a]
                for n in range(n_cols):
                    part = part + mm(left_buf[a, 2 * n], col_buf[n, a, 1])
                    part = part - mm(left_buf[a, 2 * n + 1], col_buf[n, a, 0])
                total[a] = part
            out = pltpu.make_async_copy(total, total_out, sems.at[0])
            out.start()
            for off_s, save in saves:
                pl.when(off_s < DIAGS)(save.wait)
            out.wait()

    first = 1 + n_cols
    total, keep_col = pl.pallas_call(
        kernel,
        in_specs=[place_spec()] + [any_spec()] * (n_cols + 3),
        out_specs=[any_spec()] * 2,
        out_shape=[
            jax.ShapeDtypeStruct(total_in.shape, total_in.dtype),
            jax.ShapeDtypeStruct(keep_col.shape, keep_col.dtype),
        ],
        input_output_aliases={first: 0, first + 1: 1},
        scratch_shapes=[
            pltpu.VMEM((n_cols, count, 2, bs, bs), jnp.bfloat16),
            pltpu.VMEM(lefts.shape, jnp.bfloat16),
            pltpu.VMEM((count, bs, bs), jnp.float32),
            pltpu.SemaphoreType.DMA((2 + n_cols,)),
        ],
        compiler_params=pltpu.CompilerParams(vmem_limit_bytes=VMEM_BYTES),
        cost_estimate=pl.CostEstimate(
            flops=count * 4 * 2 * bs**3, bytes_accessed=count * 12 * bs * bs * 2, transcendentals=0
        ),
        name="rest_late" if late else "sum_rest",
    )(place, *[x for x, _, _ in columns], total_in, keep_col, lefts)
    return total, keep_row, keep_col


def halves(value):
    high = value.astype(jnp.bfloat16)
    return high, (value - high.astype(jnp.float32)).astype(jnp.bfloat16)


def solve_stage(
    stage, place, output, carried, sums, late_sums, row_new, col_new, far_pairs, own_pairs, spacing, rows, cols
):
    count, bs = sums[0].shape[0], sums[0].shape[1]
    block_cols = output.shape[1]
    last = stage == DIAGS - 1
    two = last and late_sums is not None
    groups = [list(sums)] + ([list(late_sums)] if two else [])
    flat = [x for group in groups for x in group]
    n_new = len(row_new)

    passed = [] if carried is None else [carried]

    def kernel(place, out_in, *refs):
        refs = refs[len(passed) :]
        sum_groups, refs = refs[: len(flat)], refs[len(flat) :]
        row_in, refs = refs[:n_new], refs[n_new:]
        col_in, refs = refs[:n_new], refs[n_new:]
        pair_far, pair_own, space_in, out, sent, refs = *refs[:5], refs[5:]
        total, keep_r, keep_c, row_buf, col_buf, far_buf, own_buf, space, solved, narrow, sems = refs
        r, c = place[0], place[1]
        lag = lag_of(r, c, cols)
        is_late = (lax.rem(r, 2) == 1) & (lag == cols - 1)

        @pl.when(lag == stage)
        def _():
            sem = 0

            def plan(src, dst):
                nonlocal sem
                copy = pltpu.make_async_copy(src, dst, sems.at[sem])
                sem += 1
                return copy

            news = []
            for n in range(n_new):
                news.append(plan(row_in[n], row_buf.at[n]))
                news.append(plan(col_in[n], col_buf.at[n]))
            rest = [
                plan(pair_own.at[pl.ds(0, count)], own_buf),
                plan(pair_far, far_buf),
                plan(space_in, space),
            ]
            near = pl.ds(0, max(stage, 1))
            targets = [(0, total)]
            if n_new:
                targets += [(1, keep_r.at[:, near]), (2, keep_c.at[:, near])]
            first_sem = sem

            def load(group, i, dst):
                src = group[i].at[:, near] if i else group[i]
                return pltpu.make_async_copy(src, dst, sems.at[first_sem + i])

            for at, group in enumerate([sum_groups[:3], sum_groups[3:]][: len(groups)]):
                chosen = is_late if at == 1 else jnp.logical_not(is_late)
                for i, dst in targets:
                    if two:
                        pl.when(chosen)(load(group, i, dst).start)
                    else:
                        load(group, i, dst).start()
            for copy in news + rest:
                copy.start()
            for i, dst in targets:
                load(sum_groups, i, dst).wait()
            for copy in news:
                copy.wait()
            lead = lead_of(r, c, cols)
            wrapped = jnp.where(r + lag >= rows, 1, 0)
            each = range(count)
            right = [total[a] for a in each]
            for n in range(n_new):
                g = stage - n
                for a in each:
                    at = jnp.where(r + g >= rows, jnp.minimum(a + 1, count - 1), a)
                    right[a] = right[a] + mm(row_buf[n, a], keep_c[a, g - 1])
                    right[a] = right[a] - mm(keep_r[a, g - 1], col_buf[n, at])
            far = [jnp.minimum(a + wrapped, count - 1) for a in each]
            for copy in rest:
                copy.wait()

            def from_left(side, values):
                left = [halves(own_buf[a, side]) for a in each]
                value = [halves(x) for x in values]
                return [
                    mm(left[a][0], value[a][0])
                    + (mm(left[a][0], value[a][1]) + mm(left[a][1], value[a][0]))
                    for a in each
                ]

            def from_right(values, side):
                value = [halves(x) for x in values]
                return [
                    mm(value[a][0], far_buf[far[a], side]) + mm(value[a][1], far_buf[far[a], side])
                    for a in each
                ]

            mixed = from_right(from_left(1, right), 0)
            mixed = [mixed[a] / space[a] for a in each]
            answer = from_right(from_left(0, mixed), 1)
            for a in each:
                narrow[a] = answer[a].astype(jnp.bfloat16)
                solved[a] = answer[a]
            copies = []
            send = None
            if not last:
                send = pltpu.make_async_copy(narrow, sent, sems.at[sem])
                send.start()
            for a in range(count):
                at = (rows // cols) * a + FIRST // cols + lead
                copy = pltpu.make_async_copy(
                    solved.at[a], out.at[a, jnp.minimum(at, block_cols - 1)], sems.at[a]
                )
                pl.when(at < block_cols)(copy.start)
                copies.append((at, copy))
            for at, copy in copies:
                pl.when(at < block_cols)(copy.wait)
            if send is not None:
                send.wait()

    n_in = 2 + len(passed) + len(flat) + 2 * n_new + 3
    half = max(n_new, 1)
    return pl.pallas_call(
        kernel,
        in_specs=[place_spec()] + [any_spec()] * (n_in - 1),
        out_specs=[any_spec()] * 2,
        out_shape=[
            jax.ShapeDtypeStruct(output.shape, output.dtype),
            jax.ShapeDtypeStruct((count, bs, bs), jnp.bfloat16),
        ],
        input_output_aliases={1 + i: i for i in range(1 + len(passed))},
        scratch_shapes=[
            pltpu.VMEM((count, bs, bs), jnp.float32),
            pltpu.VMEM((count, DIAGS - 1, bs, bs), jnp.bfloat16),
            pltpu.VMEM((count, DIAGS - 1, bs, bs), jnp.bfloat16),
            pltpu.VMEM((half, count, bs, bs), jnp.bfloat16),
            pltpu.VMEM((half, count, bs, bs), jnp.bfloat16),
            pltpu.VMEM((count, 2, bs, bs), jnp.bfloat16),
            pltpu.VMEM((count, 2, bs, bs), jnp.float32),
            pltpu.VMEM((count, bs, bs), jnp.float32),
            pltpu.VMEM((count, bs, bs), jnp.float32),
            pltpu.VMEM((count, bs, bs), jnp.bfloat16),
            pltpu.SemaphoreType.DMA((2 * n_new + 6 + count,)),
        ],
        compiler_params=pltpu.CompilerParams(vmem_limit_bytes=VMEM_BYTES),
        cost_estimate=pl.CostEstimate(
            flops=count * 12 * 2 * bs**3, bytes_accessed=count * 20 * bs * bs * 2, transcendentals=0
        ),
    )(place, output, *passed, *flat, *row_new, *col_new, far_pairs, own_pairs, spacing)


def banded_body(schur_blocks, known_blocks, eigen_pairs, eigenvalues):
    return banded_steps(schur_blocks, known_blocks, eigen_pairs, eigenvalues)


def banded_steps(schur_blocks, known_blocks, eigen_pairs, eigenvalues):
    rows = lax.axis_size("row")
    cols = lax.axis_size("col")
    r = lax.axis_index("row")
    c = lax.axis_index("col")
    schur = schur_blocks[:, 0, :, 0]
    known = known_blocks[:, 0, :, 0]
    pairs = eigen_pairs[:, 0]
    count = known.shape[0] - 1
    chips = rows // 2
    devices = [(i, k) for i in range(rows) for k in range(cols)]

    def lag(i, k):
        return (k - i) % cols

    def send(block, move, keep=lambda i, k: True, senders=None):
        routes = []
        for i, k in devices:
            if senders is not None and lag(i, k) not in senders:
                continue
            to = move(i, k)
            to = (to[0] % rows, to[1] % cols)
            if keep(*to):
                routes.append((i * cols + k, to[0] * cols + to[1]))
        return lax.ppermute(block, ("row", "col"), routes)

    def late_core(i, k):
        return lag(i, k) == cols - 1 and i % 2 == 1

    place = jnp.stack([r, c]).astype(jnp.int32)
    col_packs = pack(known, schur, place, 0, rows, cols, "cols")
    packed = pack(known, schur, place, 0, rows, cols, "rows")
    own_parts, own_far = packed[:-1], packed[-1]
    early = {0: col_packs[0]}
    for step in range(1, chips):
        early[step] = send(col_packs[step], lambda i, j, s=step: (i - 2 * s, j))
    row_parts = [list(own_parts)]
    for k in (1, 2):
        row_parts.append([send(part, lambda i, j, k=k: (i, j ^ k)) for part in own_parts])
    row_parts.append(
        [
            send(row_parts[1][0], lambda i, j: (i, j ^ 2)),
            send(row_parts[2][1], lambda i, j: (i, j ^ 1)),
        ]
    )
    row_far, col_far = [], []
    for g in range(1, DIAGS - 1):
        takes = lambda i, k, g=g: lag(i, k) > g
        row_far.append(send(own_far, lambda i, j, g=g: (i, j + g), takes))
        col_far.append(send(own_far, lambda i, j, g=g: (i - g, j), takes))
    pair_list = [lax.optimization_barrier((pairs, own_far))[0][1:].astype(jnp.bfloat16)]
    for g in range(1, DIAGS):
        takes = lambda i, k, g=g: lag(i, k) == g
        pair_list.append(send(pair_list[-1], lambda i, j: (i - 1, j), takes))
    lag_here = lag_of(r, c, cols)
    own_ids = jnp.arange(count, dtype=jnp.int32) * rows + r
    far_ids = jnp.minimum(own_ids + FIRST + lag_here, eigenvalues.shape[0] - 1)
    spacing = eigenvalues[own_ids][:, :, None] - eigenvalues[far_ids][:, None, :]
    known_later, spacing = lax.optimization_barrier((known, spacing))
    late_packs = pack(known, schur, place, 1, rows, cols, "late")
    output = copy_blocks(known_later)

    crossed = {n: send(early[n], lambda i, j: (i ^ 1, j)) for n in range(chips)}
    late = [(late_packs[0], 0, False)]
    late_last = []
    for step in range(chips):

        def onward(i, j, step=step):
            return i - 2 * (step if j < cols // 2 else -step), j

        def onward_across(i, j, onward=onward):
            return onward(i, j)[0] ^ 1, j

        into = late_last if step else late
        if step:
            into.append((send(late_packs[step], onward, late_core), step, False))
        into.append((send(late_packs[step], onward_across, late_core), step, True))
    final = chips // 2
    last = [(early[final], final, False), (crossed[final], final, True)]
    ready = []
    for step in range(chips):
        if step != final:
            ready += [(early[step], step, False), (crossed[step], step, True)]
    sums = sum_base(
        place, row_parts, ready, [x[1:] for x in last], own_far, row_far, col_far, False, rows, cols
    )
    sums = sum_rest(place, last, sums, False, rows, cols)
    late_sums = sum_base(
        place, row_parts, late, [x[1:] for x in late_last], own_far, row_far, col_far, True, rows, cols
    )
    late_sums = sum_rest(place, late_last, late_sums, True, rows, cols)
    carried = None
    row_new = {}
    col_new = {}
    for stage in range(DIAGS):
        output, carried = solve_stage(
            stage,
            place,
            output,
            carried,
            sums,
            late_sums,
            [row_new[n, stage] for n in range(stage)],
            [col_new[n, stage] for n in range(stage)],
            pair_list[stage],
            pairs,
            spacing,
            rows,
            cols,
        )
        for hops in ROUNDS.get(stage, ()):
            by_lag = dict(hops)
            takes = set(by_lag.values())

            def gap(i, k):
                return by_lag.get(lag(i, k), lag(i, k)) - lag(i, k)

            def wanted(i, k):
                return lag(i, k) in takes

            across = send(carried, lambda i, j: (i, j + gap(i, j)), wanted, by_lag)
            upward = send(carried, lambda i, j: (i - gap(i, j), j), wanted, by_lag)
            for hop in hops:
                row_new[hop] = across
                col_new[hop] = upward
    return output[:, None, :, None]


def solution(mesh):
    rows, cols = mesh.shape["row"], mesh.shape["col"]
    banded = rows == FIRST and cols == DIAGS
    return jax.shard_map(
        banded_body if banded else body,
        mesh=mesh,
        in_specs=(
            P(None, "row", None, "col", None, None),
            P(None, "row", None, "col", None, None),
            P(None, "row", None, None, None),
            P(),
        ),
        out_specs=P(None, "row", None, "col", None, None),
        check_vma=False,
    )
```
